256 devices in a mesh: groups: 2 (over y), patch: 16 (over z), sub: 8 (over x, core).
Axes of the slice: x: 4, y: 2, z: 16, core: 2. Of those that a mesh axis runs over, the one named last changes fastest.
The devices are a block of a 4x16x16 slice.
Arguments:
- fine_nodes: float32 [262144, 128], P(('groups', 'patch', 'sub')), parts along dimension 0, may hold values from -6 to 6
- fine_edges: float32 [262144, 6, 128], P(('groups', 'patch', 'sub')), parts along dimension 0, may hold values from -6 to 6
- fine_senders: int32 [262144, 6], P(('groups', 'patch', 'sub')), parts along dimension 0, may hold values from 0 to 1279
- fine_halo: int32 [512, 128], P(('groups', 'patch', 'sub')), parts along dimension 0, may hold values from 0 to 1023
- fine_pool: int32 [262144], P(('groups', 'patch', 'sub')), parts along dimension 0, may hold values from 0 to 2047, as said below
- quarter_edges: float32 [65536, 4, 128], P(('groups', 'patch')), parts along dimension 0, may hold values from -6 to 6
- quarter_senders: int32 [65536, 4], P(('groups', 'patch')), parts along dimension 0, may hold values from 0 to 2303
- quarter_halo: int32 [64, 128], P(('groups', 'patch')), parts along dimension 0, may hold values from 0 to 2047
- quarter_pool: int32 [65536], P(('groups', 'patch')), parts along dimension 0, may hold values from 0 to 511, as said below
- coarse_edges: float32 [16384, 4, 128], P(('groups', 'patch', 'sub')), parts along dimension 0, may hold values from -6 to 6
- coarse_senders: int32 [16384, 4], P('groups'), parts along dimension 0, may hold values from 0 to 8191
- edge_in: float32 [3, 384, 128], replicated, may hold values from -0.3125 to 0.3125
- edge_out: float32 [3, 128, 128], replicated, may hold values from -0.5 to 0.5
- node_in: float32 [3, 256, 128], replicated, may hold values from -0.375 to 0.375
- node_out: float32 [3, 128, 128], replicated, may hold values from -0.5 to 0.5
Outputs:
- fine_out: float32 [262144, 128], P(('groups', 'patch', 'sub')), parts along dimension 0
The draws below stay inside these ranges and needn't reach their ends.
There are 2 independent parts, one for each index of `groups`. The reference program is written for one: setup_inputs(seed, part) draws one part's arguments, and reference() takes and returns one part's arrays. A program takes and returns all parts, laid end to end along the dimension named above; an argument that names none is the same for every part. Nothing has to cross between parts.
Inputs may be any that keep to these rules, and one draw needn't show every extreme that they name: `fine_pool`: every one of a patch's 2048 quarter nodes is the target of at least one fine node of that patch. `quarter_pool`: every one of a patch's 512 sixteenth nodes is the target of at least one quarter node of that patch.
All inputs are finite; a program needn't handle non-finite values.
Results may differ from the reference program's by a relative error of at most 0.00005.
Values sent between devices are 32-bit elements; how exact they have to be, the bound alone decides.
A program may use at most 128 MiB of HBM per device.

```python
import jax
import jax.numpy as jnp
from jax import lax

W = 128
NF_DEV = 1024
K_F = 6
K_Q = 4
K_S = 4
HALO = 128
HALO_Q = 128
QUARTER_PATCH = 2048
SIXTEENTH_PATCH = 512
NF = 131072
NQ = 32768
NS = 8192
N_PATCH = 16
N_SUB = 8


def covering(key, blocks, block_size, targets):

    def one_block(block_key):
        first_key, second_key = jax.random.split(block_key)
        extra = jax.random.randint(first_key, (block_size - targets,), 0, targets, dtype=jnp.int32)
        labels = jnp.concatenate([jnp.arange(targets, dtype=jnp.int32), extra])
        return jax.random.permutation(second_key, labels)
    block_keys = jax.random.split(key, blocks)
    return jax.vmap(one_block)(block_keys).reshape(-1)


def draw_fine_pool(key, part):
    return covering(jax.random.fold_in(key, 11), NF // (4 * QUARTER_PATCH), 4 * QUARTER_PATCH, QUARTER_PATCH)


def draw_quarter_pool(key, part):
    return covering(jax.random.fold_in(key, 23), NQ // (4 * SIXTEENTH_PATCH), 4 * SIXTEENTH_PATCH, SIXTEENTH_PATCH)


def plant(entries, rng, low, largest):
    shape = entries.shape
    index_at = [jax.random.randint(jax.random.fold_in(rng, axis), (), 0, shape[axis]) for axis in range(len(shape))]
    entries = entries.at[tuple(index_at)].set(low)
    longest = shape.index(max(shape))
    index_at[longest] = (index_at[longest] + 1) % shape[longest]
    return entries.at[tuple(index_at)].set(largest)


def block_scale(stream_key, extent, shards, low, largest):
    level = 1.0
    for position, parts in shards:
        heights = jax.random.uniform(jax.random.fold_in(jax.random.fold_in(stream_key, 6), position), (parts,), jnp.float32, low / len(shards), largest / len(shards))
        level = level * jnp.repeat(jnp.exp(heights), extent[position] // parts).reshape((-1,) + (1,) * (len(extent) - 1 - position))
    return level


def gaussian(key, shape, scale, limit, pieces=(), kind=jnp.bfloat16):
    loudness = block_scale(key, shape, pieces, -0.22, 0.18) if pieces else 1.0
    values = jax.random.normal(key, shape, jnp.float32) * scale * loudness
    return jnp.minimum(jnp.maximum(values, -limit), limit).astype(kind)


def setup_inputs(seed: int = 0, part: int = 0) -> dict:
    streams_of = jax.random.split(jax.random.key(seed), 16)
    part_splits = jax.random.split(jax.random.fold_in(streams_of[15], part), 16)
    return {
        "fine_nodes": gaussian(part_splits[0], (NF, W), 1.0, 6.0, ((0, 128),), jnp.float32),
        "fine_edges": gaussian(part_splits[1], (NF, K_F, W), 1.0, 6.0, ((0, 128),), jnp.float32),
        "fine_senders": plant(jax.random.randint(part_splits[2], (NF, K_F), 0, NF_DEV + 2 * HALO), jax.random.fold_in(part_splits[2], 1), 0, (NF_DEV + 2 * HALO) - 1).astype(jnp.int32),
        "fine_halo": plant(jax.random.randint(part_splits[3], (2 * N_PATCH * N_SUB, HALO), 0, NF_DEV), jax.random.fold_in(part_splits[3], 1), 0, NF_DEV - 1).astype(jnp.int32),
        "fine_pool": draw_fine_pool(jax.random.fold_in(jax.random.fold_in(streams_of[15], part), 71), part),
        "quarter_edges": gaussian(part_splits[5], (NQ, K_Q, W), 1.0, 6.0, ((0, 16),), jnp.float32),
        "quarter_senders": plant(jax.random.randint(part_splits[6], (NQ, K_Q), 0, QUARTER_PATCH + 2 * HALO_Q), jax.random.fold_in(part_splits[6], 1), 0, (QUARTER_PATCH + 2 * HALO_Q) - 1).astype(jnp.int32),
        "quarter_halo": plant(jax.random.randint(part_splits[7], (2 * N_PATCH, HALO_Q), 0, QUARTER_PATCH), jax.random.fold_in(part_splits[7], 1), 0, QUARTER_PATCH - 1).astype(jnp.int32),
        "quarter_pool": draw_quarter_pool(jax.random.fold_in(jax.random.fold_in(streams_of[15], part), 71), part),
        "coarse_edges": gaussian(part_splits[9], (NS, K_S, W), 1.0, 6.0, ((0, 128),), jnp.float32),
        "coarse_senders": plant(jax.random.randint(part_splits[10], (NS, K_S), 0, NS), jax.random.fold_in(part_splits[10], 1), 0, NS - 1).astype(jnp.int32),
        "edge_in": gaussian(streams_of[11], (3, 3 * W, W), (3 * W) ** -0.5, 0.3125, (), jnp.float32),
        "edge_out": gaussian(streams_of[12], (3, W, W), W ** -0.5, 0.5, (), jnp.float32),
        "node_in": gaussian(streams_of[13], (3, 2 * W, W), (2 * W) ** -0.5, 0.375, (), jnp.float32),
        "node_out": gaussian(streams_of[14], (3, W, W), W ** -0.5, 0.5, (), jnp.float32),
    }


exact_mode = lax.Precision.HIGHEST

def product(left, right):
    return jnp.dot(left, right, precision=exact_mode)

def normalize(values):
    centred = values - lax.optimization_barrier(jnp.mean(values, axis=-1, keepdims=True))
    spread = lax.optimization_barrier(jnp.mean(centred * centred, axis=-1, keepdims=True))
    return centred * lax.rsqrt(spread + 1e-05)

def process_level(receivers, sources, senders, edge_feats, edge_in, edge_out, node_in, node_out):
    rows_count, degree, width = edge_feats.shape
    sender_proj = product(sources, edge_in[:width])
    receiver_proj = product(receivers, edge_in[width:2 * width])
    edge_proj = product(edge_feats.reshape(rows_count * degree, width), edge_in[2 * width:]).reshape(rows_count, degree, width)
    hidden = jax.nn.relu(sender_proj[senders] + receiver_proj[:, None, :] + edge_proj)
    message = product(hidden.reshape(rows_count * degree, width), edge_out).reshape(rows_count, degree, width)
    summed = lax.optimization_barrier(jnp.sum(edge_feats + normalize(message), axis=1))
    node_hidden = jax.nn.relu(product(receivers, node_in[:width]) + product(summed, node_in[width:]))
    return receivers + normalize(product(node_hidden, node_out))

def halo_rows_global(halo_lists, blocks, block_size, margin):
    lists = halo_lists.reshape(blocks, 2, margin)
    starts = jnp.arange(blocks, dtype=jnp.int32) * block_size
    own_rows = starts[:, None] + jnp.arange(block_size, dtype=jnp.int32)[None, :]
    from_left = jnp.roll(starts, 1)[:, None] + jnp.roll(lists[:, 0], 1, axis=0)
    from_right = jnp.roll(starts, -1)[:, None] + jnp.roll(lists[:, 1], -1, axis=0)
    return jnp.concatenate([own_rows, from_left, from_right], axis=1)

def global_senders(senders, lookup):
    blocks = lookup.shape[0]
    local_ids = senders.reshape(blocks, -1, senders.shape[1])
    picked = jax.vmap(lambda rows_here, picks: rows_here[picks])(lookup, local_ids)
    return picked.reshape(senders.shape)

def pool_mean(values, targets, segments):
    sums = jax.ops.segment_sum(values, targets, num_segments=segments)
    counts = jax.ops.segment_sum(jnp.ones((values.shape[0],), jnp.float32), targets, num_segments=segments)
    return sums / counts[:, None]

def reference(fine_nodes, fine_edges, fine_senders, fine_halo, fine_pool, quarter_edges, quarter_senders, quarter_halo, quarter_pool, coarse_edges, coarse_senders, edge_in, edge_out, node_in, node_out):
    fine_lookup = halo_rows_global(fine_halo, N_PATCH * N_SUB, NF_DEV, HALO)
    fine_new = process_level(fine_nodes, fine_nodes, global_senders(fine_senders, fine_lookup), fine_edges, edge_in[0], edge_out[0], node_in[0], node_out[0])
    fine_owner = jnp.arange(NF, dtype=jnp.int32) // (NF_DEV * N_SUB)
    fine_target = fine_owner * QUARTER_PATCH + fine_pool
    quarter_nodes = pool_mean(fine_new, fine_target, NQ)
    quarter_lookup = halo_rows_global(quarter_halo, N_PATCH, QUARTER_PATCH, HALO_Q)
    quarter_new = process_level(quarter_nodes, quarter_nodes, global_senders(quarter_senders, quarter_lookup), quarter_edges, edge_in[1], edge_out[1], node_in[1], node_out[1])
    quarter_owner = jnp.arange(NQ, dtype=jnp.int32) // QUARTER_PATCH
    quarter_target = quarter_owner * SIXTEENTH_PATCH + quarter_pool
    coarse_nodes = pool_mean(quarter_new, quarter_target, NS)
    coarse_new = process_level(coarse_nodes, coarse_nodes, coarse_senders, coarse_edges, edge_in[2], edge_out[2], node_in[2], node_out[2])
    quarter_out = quarter_new + coarse_new[quarter_target]
    return fine_new + quarter_out[fine_target]
```

```python
import functools

import jax
import jax.numpy as jnp
from jax import lax
from jax.experimental import pallas as pl
from jax.experimental.pallas import tpu as pltpu
from jax.sharding import PartitionSpec as P

MESH = pl.DeviceIdType.MESH
BF = jnp.bfloat16
F32 = jnp.float32
W = 128
VMEM_LIMIT = 56 * 1024 * 1024


def split2(x):
    hi = x.astype(BF)
    lo = (x - hi.astype(F32)).astype(BF)
    return jnp.concatenate([hi, lo], axis=1)


def packed(w):
    s = split2(w)
    return jnp.concatenate([s, s], axis=0)


def halves(y):
    return y[:, :W] + y[:, W:]


def dot(a, b):
    return jnp.dot(a, b, preferred_element_type=F32)


def mm(x, wp):
    return halves(dot(split2(x), wp))


def centred_columns(w):
    return w - jnp.mean(w, axis=1, keepdims=True)


def scaled(m):
    return m * lax.rsqrt(jnp.mean(m * m, axis=1, keepdims=True) + 1e-05)


def column(row):
    return jnp.broadcast_to(row, (W, W)).T


def lanes(rows):
    return lax.broadcasted_iota(jnp.int32, (rows, W), 1)


def sublanes(rows):
    return lax.broadcasted_iota(jnp.int32, (rows, W), 0)


def ones_where(mask):
    return jnp.where(mask, 1.0, 0.0).astype(BF)


def one_hot(col, width):
    lane = lanes(col.shape[0])
    return jnp.concatenate([ones_where(col == lane + j * W) for j in range(width // W)], axis=1)


def one_hot_t(index_ref, first, rows, blocks):
    sub = sublanes(rows) + first
    return jnp.concatenate(
        [ones_where(jnp.broadcast_to(index_ref[j : j + 1, :], (rows, W)) == sub) for j in range(blocks)],
        axis=1,
    )


def counts_of(index_ref, first, rows, blocks):
    sub = sublanes(rows) + first

    def add(j, acc):
        row = jnp.broadcast_to(index_ref[pl.ds(j, 1), :], (rows, W))
        return acc + jnp.where(row == sub, 1.0, 0.0)

    acc = lax.fori_loop(0, blocks, add, jnp.zeros((rows, W), F32))
    return jnp.sum(acc, axis=1, keepdims=True)


def halo_kernel(n_patch, n_sub, nodes, halo, pool, rows_out, pool_out,
                nodes_v, sent, got, pools, node_sem, send, recv, psend, precv):
    p, s = lax.axis_index("patch"), lax.axis_index("sub")
    fetch = pltpu.make_async_copy(nodes, nodes_v, node_sem)
    fetch.start()
    after = {"patch": lax.rem(p + (s + 1) // n_sub, n_patch), "sub": lax.rem(s + 1, n_sub)}
    wrap = (n_sub - s) // n_sub
    before = {"patch": lax.rem(p + n_patch - wrap, n_patch), "sub": lax.rem(s + n_sub - 1, n_sub)}
    peers = [{"sub": lax.rem(s + r, n_sub)} for r in range(1, n_sub)]
    barrier = pltpu.get_barrier_semaphore()
    for to in [after, before] + peers:
        pl.semaphore_signal(barrier, inc=1, device_id=to, device_id_type=MESH)
    count = pool.shape[0]
    pools[pl.ds(pl.multiple_of(s * count, count), count), :] = pool[...]
    pl.semaphore_wait(barrier, n_sub + 1)
    pool_copies = []
    for r, to in enumerate(peers):
        place = pools.at[pl.ds(pl.multiple_of(s * count, count), count), :]
        c = pltpu.make_async_remote_copy(place, place, psend.at[r], precv.at[r], device_id=to, device_id_type=MESH)
        c.start()
        pool_copies.append(c)
    fetch.wait()
    table = split2(nodes_v[...])
    copies = []
    for k, to in ((0, after), (1, before)):
        sent[k] = halves(dot(one_hot(column(halo[k : k + 1, :]), nodes_v.shape[0]), table))
        c = pltpu.make_async_remote_copy(sent.at[k], got.at[k], send.at[k], recv.at[k], device_id=to, device_id_type=MESH)
        c.start()
        copies.append(c)
    for c in pool_copies + copies:
        c.wait()
    rows_out[0:W, :] = got[0]
    rows_out[W : 2 * W, :] = got[1]
    pool_out[...] = pools[...]


def fine_halo_exchange(n_patch, n_sub, nodes, halo, pool):
    any_ = pl.BlockSpec(memory_space=pl.ANY)
    vm = pl.BlockSpec(memory_space=pltpu.VMEM)
    return pl.pallas_call(
        functools.partial(halo_kernel, n_patch, n_sub),
        name="fine_halo",
        out_shape=(
            jax.ShapeDtypeStruct((2 * W, W), F32),
            jax.ShapeDtypeStruct((n_sub * pool.shape[0], W), jnp.int32),
        ),
        in_specs=[any_, vm, vm],
        out_specs=(vm, vm),
        scratch_shapes=[
            pltpu.VMEM(nodes.shape, F32),
            pltpu.VMEM((2, W, W), F32),
            pltpu.VMEM((2, W, W), F32),
            pltpu.VMEM((n_sub * pool.shape[0], W), jnp.int32),
            pltpu.SemaphoreType.DMA,
            pltpu.SemaphoreType.DMA((2,)),
            pltpu.SemaphoreType.DMA((2,)),
            pltpu.SemaphoreType.DMA((n_sub - 1,)),
            pltpu.SemaphoreType.DMA((n_sub - 1,)),
        ],
        compiler_params=pltpu.CompilerParams(collective_id=0, has_side_effects=True, vmem_limit_bytes=VMEM_LIMIT),
    )(nodes, halo, pool)


TILE = 128


def fine_kernel(nodes, halo, senders, edges, pool, edge_in, edge_out, node_in, node_out,
                new_out, sums_out, table, recv_w, out_w, node_w, last_w, news):
    step = pl.program_id(0)
    degree = edges.shape[0]
    n_src = nodes.shape[0]
    n_halo = halo.shape[0]
    width = n_src + n_halo

    @pl.when(step == 0)
    def _():
        send_w = packed(edge_in[0:W, :])
        for j in range(n_src // 256):
            table[j * 256 : (j + 1) * 256, :] = split2(mm(nodes[j * 256 : (j + 1) * 256, :], send_w))
        table[n_src:width, :] = split2(mm(halo[...], send_w))
        table[width : width + 2 * W, :] = packed(edge_in[2 * W : 3 * W, :])
        recv_w[...] = packed(edge_in[W : 2 * W, :])
        out_w[...] = packed(centred_columns(edge_out[...]))
        node_w[0 : 2 * W, :] = packed(node_in[0:W, :])
        node_w[2 * W : 4 * W, :] = packed(node_in[W : 2 * W, :])
        last_w[...] = packed(centred_columns(node_out[...]))

    start = pl.multiple_of(step * TILE, TILE)
    h = nodes[pl.ds(start, TILE), :]
    h2 = split2(h)
    received = halves(dot(h2, recv_w[...]))
    left = jnp.concatenate(
        [
            jnp.concatenate([one_hot(column(senders[k : k + 1, :]), width), split2(edges[k])], axis=1)
            for k in range(degree)
        ],
        axis=0,
    )
    hidden = halves(dot(left, table[...]))
    hidden = jnp.maximum(hidden + jnp.concatenate([received] * degree, axis=0), 0.0)
    message = scaled(mm(hidden, out_w[...]))
    summed = edges[0] + message[0:TILE]
    for k in range(1, degree):
        summed = summed + (edges[k] + message[k * TILE : (k + 1) * TILE])
    node_hidden = jnp.maximum(halves(dot(jnp.concatenate([h2, split2(summed)], axis=1), node_w[...])), 0.0)
    new = h + scaled(mm(node_hidden, last_w[...]))
    new_out[...] = new
    news[pl.ds(start, TILE), :] = split2(new)

    @pl.when(step == pl.num_programs(0) - 1)
    def _():
        blocks = pool.shape[0]

        def some(q, carry):
            first = pl.multiple_of(q * 256, 256)
            sums_out[pl.ds(first, 256), :] = halves(dot(one_hot_t(pool, first, 256, blocks), news[...]))
            return carry

        lax.fori_loop(0, sums_out.shape[0] // 256, some, 0)


def fine_level(nodes, halo, senders, edges, pool, edge_in, edge_out, node_in, node_out, targets):
    degree, rows, _ = edges.shape
    whole = lambda a: pl.BlockSpec(a.shape, lambda i: (0,) * a.ndim)
    level = lambda a: pl.BlockSpec((None,) + a.shape[1:], lambda i: (0, 0, 0))
    return pl.pallas_call(
        fine_kernel,
        name="fine_level",
        grid=(rows // TILE,),
        out_shape=(jax.ShapeDtypeStruct((rows, W), F32), jax.ShapeDtypeStruct((targets, W), F32)),
        in_specs=[
            whole(nodes),
            whole(halo),
            pl.BlockSpec((degree, TILE), lambda i: (0, i)),
            pl.BlockSpec((degree, TILE, W), lambda i: (0, i, 0)),
            whole(pool),
            level(edge_in),
            level(edge_out),
            level(node_in),
            level(node_out),
        ],
        out_specs=(
            pl.BlockSpec((TILE, W), lambda i: (i, 0)),
            pl.BlockSpec((targets, W), lambda i: (0, 0)),
        ),
        scratch_shapes=[
            pltpu.VMEM((rows + halo.shape[0] + 2 * W, 2 * W), BF),
            pltpu.VMEM((2 * W, 2 * W), BF),
            pltpu.VMEM((2 * W, 2 * W), BF),
            pltpu.VMEM((4 * W, 2 * W), BF),
            pltpu.VMEM((2 * W, 2 * W), BF),
            pltpu.VMEM((rows, 2 * W), BF),
        ],
        compiler_params=pltpu.CompilerParams(vmem_limit_bytes=VMEM_LIMIT),
    )(nodes, halo, senders, edges, pool, edge_in, edge_out, node_in, node_out)


def node_update(h, summed, node_in, node_out):
    a = jnp.maximum(mm(h, packed(node_in[0:W, :])) + mm(summed, packed(node_in[W : 2 * W, :])), 0.0)
    return h + scaled(mm(a, packed(centred_columns(node_out))))


def coarse_kernel(n_patch, n_sub,
                  sums, pools, q_edges, q_senders, q_halo, q_pool, c_edges, c_senders, edge_in, edge_out, node_in,
                  node_out, qall_out, ctab_out,
                  sums_v, qe_v, ce_v, qs_v, cs_v, ei_v, eo_v, ni_v, no_v,
                  pair_buf, comb, rs_buf, tab, hsent, qall, p16, r16, zt, gsend, gbuf, ctab,
                  load_sem, pair_s, pair_r, rs_s, rs_r, ag_s, ag_r, agf_s, agf_r, h_s, h_r,
                  qg_s, qg_r, qgf_s, qgf_r, t_s, t_r, z_s, z_r, d_s, d_r, g_s, g_r, c_s, c_r):
    p, me = lax.axis_index("patch"), lax.axis_index("sub")
    core = lax.rem(me, 2)
    x = me // 2
    n_x = n_sub // 2
    partner = {"sub": me + 1 - 2 * core}
    q_rows = sums.shape[0]
    share = q_rows // n_sub
    s_rows = p16.shape[0]
    s_share = s_rows // n_sub
    k_q = qs_v.shape[0]
    k_s = cs_v.shape[0]

    def column_of(r):
        return lax.rem(x + r, n_x)

    def device(r):
        return {"sub": 2 * column_of(r) + core}

    def patch(r):
        return {"patch": lax.rem(p + r + n_patch, n_patch)}

    def share_of(t, size=share):
        return pl.ds(pl.multiple_of(t * size, size), size)

    loads = [
        pltpu.make_async_copy(sums, sums_v, load_sem.at[0]),
        pltpu.make_async_copy(q_edges.at[share_of(me, share * k_q), :], qe_v, load_sem.at[1]),
        pltpu.make_async_copy(c_edges, ce_v, load_sem.at[2]),
        pltpu.make_async_copy(q_senders, qs_v, load_sem.at[3]),
        pltpu.make_async_copy(c_senders.at[:, share_of(p, s_rows)], cs_v, load_sem.at[4]),
        pltpu.make_async_copy(edge_in.at[pl.ds(1, 2)], ei_v, load_sem.at[5]),
        pltpu.make_async_copy(edge_out.at[pl.ds(1, 2)], eo_v, load_sem.at[6]),
        pltpu.make_async_copy(node_in.at[pl.ds(1, 2)], ni_v, load_sem.at[7]),
        pltpu.make_async_copy(node_out.at[pl.ds(1, 2)], no_v, load_sem.at[8]),
    ]
    for c in loads:
        c.start()

    barrier = pltpu.get_barrier_semaphore()
    for r in range(1, n_sub):
        pl.semaphore_signal(barrier, inc=1, device_id={"sub": lax.rem(me + r, n_sub)}, device_id_type=MESH)
    for r in (1, 2, -1, -2):
        pl.semaphore_signal(barrier, inc=1, device_id=patch(r), device_id_type=MESH)
    loads[0].wait()
    pl.semaphore_wait(barrier, n_sub + 3)

    started = []

    def send(src, dst, ss, rs, to):
        c = pltpu.make_async_remote_copy(src, dst, ss, rs, device_id=to, device_id_type=MESH)
        c.start()
        started.append(c)
        return c

    order = (2, 1, 3, 0)
    pair = {}
    for r in order:
        t = 2 * column_of(r) + 1 - core
        pair[r] = send(sums_v.at[share_of(t), :], pair_buf.at[r], pair_s.at[r], pair_r.at[r], partner)
    counts = counts_of(pools, me * share, share, pools.shape[0])
    for c in loads[1:]:
        c.wait()
    rs = {}
    for r in order:
        pair[r].wait_recv()
        t = 2 * column_of(r) + core
        comb[r] = sums_v[share_of(t), :] + pair_buf[r]
        if r:
            rs[r] = send(comb.at[r], rs_buf.at[r], rs_s.at[r], rs_r.at[r], device(r))
    send_w = packed(ei_v[0, 0:W, :])
    total = comb[0]
    for r in (1, 3, 2):
        rs[r].wait_recv()
        total = total + rs_buf[r]
    q = total / counts
    tab[share_of(me), :] = mm(q, send_w)

    def gather_all(buf, ss, rs_, fs, fr, size):
        mine = buf.at[share_of(me, size), :]
        out = {}
        for r in (2, 1, 3):
            out[r] = send(mine, mine, ss.at[r], rs_.at[r], device(r))
        fwd = [send(mine, mine, fs.at[0], fr.at[0], partner)]
        return out, fwd

    def forward_all(buf, out, fwd, fs, fr, size):
        for r in (1, 3, 2):
            out[r].wait_recv()
            t = 2 * column_of(n_x - r) + core
            block = buf.at[share_of(t, size), :]
            fwd.append(send(block, block, fs.at[r], fr.at[r], partner))
        for c in fwd:
            c.wait_recv()

    out, fwd = gather_all(tab, ag_s, ag_r, agf_s, agf_r, share)
    q_recv = mm(q, packed(ei_v[0, W : 2 * W, :]))
    base = []
    edges = []
    edge_w = packed(ei_v[0, 2 * W : 3 * W, :])
    for k in range(k_q):
        e = qe_v[pl.ds(k, share, stride=k_q), :]
        edges.append(e)
        base.append(mm(e, edge_w) + q_recv)
    forward_all(tab, out, fwd, agf_s, agf_r, share)
    table2 = split2(tab[0:q_rows, :])
    halo = []
    for k, r in ((0, 1), (1, -1)):
        hsent[k] = halves(dot(one_hot(column(q_halo[k : k + 1, :]), q_rows), table2))
        halo.append(
            send(hsent.at[k], tab.at[pl.ds(q_rows + k * W, W), :], h_s.at[k], h_r.at[k], patch(r))
        )
    own_cols = []
    for k in range(k_q):
        row = qs_v[k : k + 1, share_of(me)]
        own_cols.append(jnp.concatenate([column(row[:, j * W : (j + 1) * W]) for j in range(share // W)], axis=0))
    for k in range(k_q):
        base[k] = base[k] + halves(dot(one_hot(own_cols[k], q_rows), table2))
    for c in halo:
        c.wait_recv()
    halo2 = split2(tab[pl.ds(q_rows, 2 * W), :])
    out_w = packed(centred_columns(eo_v[0]))
    summed = None
    for k in range(k_q):
        hid = jnp.maximum(base[k] + halves(dot(one_hot(own_cols[k] - q_rows, 2 * W), halo2)), 0.0)
        term = edges[k] + scaled(mm(hid, out_w))
        summed = term if summed is None else summed + term
    q_new = node_update(q, summed, ni_v[0], no_v[0])
    qall[share_of(me), :] = q_new

    per = share // W
    sub = sublanes(s_rows)
    own_pool = q_pool[pl.ds(me * per, per), :]
    hot = jnp.concatenate(
        [ones_where(jnp.broadcast_to(own_pool[j : j + 1, :], (s_rows, W)) == sub) for j in range(per)], axis=1
    )
    p16[...] = halves(dot(hot, split2(q_new)))
    parts = {}
    for r in (4, 3, 5, 2, 6, 1, 7):
        t = lax.rem(me + r, n_sub)
        parts[r] = send(p16.at[share_of(t, s_share), :], r16.at[r], t_s.at[r], t_r.at[r], {"sub": t})
    q_out, q_fwd = gather_all(qall, qg_s, qg_r, qgf_s, qgf_r, share)
    c_counts = counts_of(q_pool, me * s_share, s_share, q_pool.shape[0])
    c_total = p16[share_of(me, s_share), :]
    for r in range(1, n_sub):
        parts[r].wait_recv()
        c_total = c_total + r16[r]
    c = c_total / c_counts
    mine = pl.ds(pl.multiple_of(core * s_share, s_share), s_share)
    zt[p, mine, :] = mm(c, packed(ei_v[1, 0:W, :]))

    arrivals = {}

    def relay(src, sign, dist, last):
        block = zt.at[src, mine, :]
        way = 0 if sign > 0 else 1
        for hop in (2, 1):
            if dist + hop <= last:
                arrivals[sign, dist + hop] = send(
                    block, block, z_s.at[way, dist + hop], z_r.at[way, dist + hop], patch(sign * hop)
                )

    shared = []

    def hand_over(src, slot):
        block = zt.at[src, mine, :]
        shared.append(send(block, block, d_s.at[slot], d_r.at[slot], partner))

    far, near = n_patch // 2, n_patch - n_patch // 2 - 1
    limits = {1: far, -1: near}
    for sign in (1, -1):
        relay(p, sign, 0, limits[sign])
    hand_over(p, 0)
    for dist in range(2, far + 2, 2):
        for d in (dist, dist - 1):
            for sign in (1, -1):
                if d <= limits[sign]:
                    arrivals[sign, d].wait_recv()
                    src = lax.rem(p - sign * d + n_patch, n_patch)
                    if d == dist:
                        relay(src, sign, d, limits[sign])
                    hand_over(src, d if sign > 0 else far + d)
    c_recv = mm(c, packed(ei_v[1, W : 2 * W, :]))
    c_edge_w = packed(ei_v[1, 2 * W : 3 * W, :])
    c_base = []
    c_edge = []
    for k in range(k_s):
        e = ce_v[pl.ds(k, s_share, stride=k_s), :]
        c_edge.append(e)
        c_base.append(mm(e, c_edge_w) + c_recv)
    for s in shared:
        s.wait_recv()
    ztable = split2(zt[...].reshape(n_patch * 2 * s_share, W))
    got = {}
    own = None
    for r in (2, 1, 3, 0):
        xr = column_of(r)
        cols = []
        for k in range(k_s):
            col = column(cs_v[k : k + 1, pl.ds(pl.multiple_of(xr * W, W), W)])
            cols.append(jnp.where(core == 0, col[0:s_share], col[s_share : 2 * s_share]))
        g = jnp.concatenate(cols, axis=0)
        here = (g // W) % n_x == x
        g = jnp.where(here, (g // s_rows) * W + g % W, -1)
        rows = halves(dot(one_hot(g, n_patch * W), ztable))
        if r:
            gsend[r] = rows
            got[r] = send(gsend.at[r], gbuf.at[r], g_s.at[r], g_r.at[r], device(r))
        else:
            own = rows
    for r in (1, 3, 2):
        got[r].wait_recv()
        own = own + gbuf[r]
    c_out_w = packed(centred_columns(eo_v[1]))
    hid = jnp.maximum(jnp.concatenate(c_base, axis=0) + own, 0.0)
    msg = scaled(mm(hid, c_out_w))
    summed = None
    for k in range(k_s):
        term = c_edge[k] + msg[k * s_share : (k + 1) * s_share]
        summed = term if summed is None else summed + term
    c_new = node_update(c, summed, ni_v[1], no_v[1])
    ctab[share_of(me, s_share), :] = c_new
    block = ctab.at[share_of(me, s_share), :]
    last = []
    for r in (4, 3, 5, 2, 6, 1, 7):
        last.append(send(block, block, c_s.at[r], c_r.at[r], {"sub": lax.rem(me + r, n_sub)}))
    forward_all(qall, q_out, q_fwd, qgf_s, qgf_r, share)
    qall_out[...] = qall[...]
    for l in last:
        l.wait_recv()
    ctab_out[...] = ctab[...]
    for s in started:
        s.wait_send()


def coarse_levels(n_patch, n_sub, sums, pools, q_edges, q_senders, q_halo, q_pool, c_edges, c_senders, edge_in,
                  edge_out, node_in, node_out):
    any_ = pl.BlockSpec(memory_space=pl.ANY)
    vm = pl.BlockSpec(memory_space=pltpu.VMEM)
    q_rows = sums.shape[0]
    share = q_rows // n_sub
    k_q, k_s = q_senders.shape[0], c_senders.shape[0]
    s_rows = c_senders.shape[1] // n_patch
    s_share = s_rows // n_sub
    n_x = n_sub // 2
    dma = pltpu.SemaphoreType.DMA
    v = lambda *shape: pltpu.VMEM(shape, F32)
    return pl.pallas_call(
        functools.partial(coarse_kernel, n_patch, n_sub),
        name="coarse_levels",
        out_shape=(jax.ShapeDtypeStruct((q_rows, W), F32), jax.ShapeDtypeStruct((s_rows, W), F32)),
        in_specs=[any_, vm, any_, any_, vm, vm, any_, any_, any_, any_, any_, any_],
        out_specs=(vm, vm),
        scratch_shapes=[
            v(q_rows, W),
            v(share * k_q, W),
            v(s_share * k_s, W),
            pltpu.VMEM((k_q, q_rows), jnp.int32),
            pltpu.VMEM((k_s, s_rows), jnp.int32),
            v(2, 3 * W, W),
            v(2, W, W),
            v(2, 2 * W, W),
            v(2, W, W),
            v(n_x, share, W),
            v(n_x, share, W),
            v(n_x, share, W),
            v(q_rows + 2 * W, W),
            v(2, W, W),
            v(q_rows, W),
            v(s_rows, W),
            v(n_sub, s_share, W),
            v(n_patch, 2 * s_share, W),
            v(n_x, s_share * k_s, W),
            v(n_x, s_share * k_s, W),
            v(s_rows, W),
            dma((9,)),
            dma((n_x,)), dma((n_x,)),
            dma((n_x,)), dma((n_x,)),
            dma((n_x,)), dma((n_x,)),
            dma((n_x,)), dma((n_x,)),
            dma((2,)), dma((2,)),
            dma((n_x,)), dma((n_x,)),
            dma((n_x,)), dma((n_x,)),
            dma((n_sub,)), dma((n_sub,)),
            dma((2, n_patch)), dma((2, n_patch)),
            dma((n_patch,)), dma((n_patch,)),
            dma((n_x,)), dma((n_x,)),
            dma((n_sub,)), dma((n_sub,)),
        ],
        compiler_params=pltpu.CompilerParams(collective_id=1, has_side_effects=True, vmem_limit_bytes=VMEM_LIMIT),
    )(sums, pools, q_edges, q_senders, q_halo, q_pool, c_edges, c_senders, edge_in, edge_out, node_in, node_out)


def last_kernel(new, qall, ctab, pool, q_pool, out, table):
    n_q, n_c = qall.shape[0], ctab.shape[0]
    c2 = split2(ctab[...])
    for j in range(n_q // W):
        hot = one_hot(column(q_pool[j : j + 1, :]), n_c)
        rows = slice(j * W, (j + 1) * W)
        table[rows, :] = split2(qall[rows, :] + halves(dot(hot, c2)))
    for j in range(new.shape[0] // 256):
        col = jnp.concatenate([column(pool[2 * j + i : 2 * j + i + 1, :]) for i in range(2)], axis=0)
        rows = slice(j * 256, (j + 1) * 256)
        out[rows, :] = new[rows, :] + halves(dot(one_hot(col, n_q), table[...]))


def last_step(new, qall, ctab, pool, q_pool):
    vm = pl.BlockSpec(memory_space=pltpu.VMEM)
    return pl.pallas_call(
        last_kernel,
        name="last_step",
        out_shape=jax.ShapeDtypeStruct(new.shape, F32),
        in_specs=[vm] * 5,
        out_specs=vm,
        scratch_shapes=[pltpu.VMEM((qall.shape[0], 2 * W), BF)],
        compiler_params=pltpu.CompilerParams(vmem_limit_bytes=VMEM_LIMIT),
    )(new, qall, ctab, pool, q_pool)


def on_device(n_patch, n_sub, fine_nodes, fine_edges, fine_senders, fine_halo, fine_pool, quarter_edges,
              quarter_senders, quarter_halo, quarter_pool, coarse_edges, coarse_senders, edge_in, edge_out, node_in,
              node_out):
    edges = fine_edges.transpose(1, 0, 2)
    pool = fine_pool.reshape(-1, W)
    q_pool = quarter_pool.reshape(-1, W)
    halo, pools = fine_halo_exchange(n_patch, n_sub, fine_nodes, fine_halo, pool)
    new, sums = fine_level(fine_nodes, halo, fine_senders.T, edges, pool, edge_in, edge_out, node_in, node_out,
                           quarter_senders.shape[0])
    qall, ctab = coarse_levels(n_patch, n_sub, sums, pools, quarter_edges.reshape(-1, W), quarter_senders.T,
                               quarter_halo, q_pool, coarse_edges.reshape(-1, W), coarse_senders.T, edge_in, edge_out,
                               node_in, node_out)
    return last_step(new, qall, ctab, pool, q_pool)


def solution(mesh):
    both = ("groups", "patch", "sub")
    halfway = ("groups", "patch")
    in_specs = (
        P(both, None),
        P(both, None, None),
        P(both, None),
        P(both, None),
        P(both),
        P(halfway, None, None),
        P(halfway, None),
        P(halfway, None),
        P(halfway),
        P(both, None, None),
        P("groups", None),
        P(),
        P(),
        P(),
        P(),
    )
    return jax.shard_map(
        functools.partial(on_device, mesh.shape["patch"], mesh.shape["sub"]),
        mesh=mesh,
        in_specs=in_specs,
        out_specs=P(both, None),
        check_vma=False,
    )
```

```python
import functools

import jax
import jax.numpy as jnp
from jax import lax
from jax.experimental import pallas as pl
from jax.experimental.pallas import tpu as pltpu
from jax.sharding import PartitionSpec as P

MESH = pl.DeviceIdType.MESH
BF = jnp.bfloat16
F32 = jnp.float32
W = 128
VMEM_LIMIT = 56 * 1024 * 1024


def split2(x):
    hi = x.astype(BF)
    lo = (x - hi.astype(F32)).astype(BF)
    return jnp.concatenate([hi, lo], axis=1)


def packed(w):
    s = split2(w)
    return jnp.concatenate([s, s], axis=0)


def halves(y):
    return y[:, :W] + y[:, W:]


def dot(a, b):
    return jnp.dot(a, b, preferred_element_type=F32)


def mm(x, wp):
    return halves(dot(split2(x), wp))


def centred_columns(w):
    return w - jnp.mean(w, axis=1, keepdims=True)


def scaled(m):
    return m * lax.rsqrt(jnp.mean(m * m, axis=1, keepdims=True) + 1e-05)


def column(row):
    return jnp.broadcast_to(row, (W, W)).T


def lanes(rows):
    return lax.broadcasted_iota(jnp.int32, (rows, W), 1)


def sublanes(rows):
    return lax.broadcasted_iota(jnp.int32, (rows, W), 0)


def ones_where(mask):
    return jnp.where(mask, 1.0, 0.0).astype(BF)


def one_hot(col, width):
    lane = lanes(col.shape[0])
    return jnp.concatenate([ones_where(col == lane + j * W) for j in range(width // W)], axis=1)


def one_hot_t(index_ref, first, rows, blocks):
    sub = sublanes(rows) + first
    return jnp.concatenate(
        [ones_where(jnp.broadcast_to(index_ref[j : j + 1, :], (rows, W)) == sub) for j in range(blocks)],
        axis=1,
    )


def counts_of(index_ref, first, rows, blocks):
    sub = sublanes(rows) + first

    def add(j, acc):
        row = jnp.broadcast_to(index_ref[pl.ds(j, 1), :], (rows, W))
        return acc + jnp.where(row == sub, 1.0, 0.0)

    acc = lax.fori_loop(0, blocks, add, jnp.zeros((rows, W), F32))
    return jnp.sum(acc, axis=1, keepdims=True)


TILE = 256


class Sends:
    def __init__(self):
        self.all = []

    def __call__(self, src, dst, ss, rs, to):
        c = pltpu.make_async_remote_copy(src, dst, ss, rs, device_id=to, device_id_type=MESH)
        c.start()
        self.all.append(c)
        return c


def node_update(h, summed, node_w, last_w):
    both = jnp.concatenate([split2(h), split2(summed)], axis=1)
    a = jnp.maximum(halves(dot(both, node_w)), 0.0)
    return h + scaled(mm(a, last_w))


def levels_kernel(n_patch, n_sub,
                  nodes, f_edges, f_senders, f_halo, pool, q_edges, q_senders, q_halo, q_pool, c_edges, c_senders,
                  edge_in, edge_out, node_in, node_out,
                  out,
                  nodes_v, fe_v, fs_v, qe_v, qs_v, ce_v, cs_v, ei_v, eo_v, ni_v, no_v,
                  pools, fh_sent, fh_got, table, news, zs, new_v,
                  sums_v, pair_buf, comb, stage, relay_in, arrive,
                  tab, hsent, qall, oh_q, oh_h, oh_c, oh_p, oh_t, base_v,
                  p16, pair16, comb16, stage16, relay16, arrive16, zt, gpart, gstage, grelay, garrive, ctab,
                  load_sem, edge_sem, fh_s, fh_r, pl_s, pl_r,
                  pair_s, pair_r, rs_s, rs_r, ag_s, ag_r, h_s, h_r,
                  pair16_s, pair16_r, rs16_s, rs16_r, qg_s, qg_r, z_s, z_r, d_s, d_r, g_s, g_r, cg_s, cg_r):
    p, me = lax.axis_index("patch"), lax.axis_index("sub")
    core = lax.rem(me, 2)
    x = me // 2
    n_x = n_sub // 2
    partner = {"sub": me + 1 - 2 * core}
    rows = nodes.shape[0]
    degree = f_edges.shape[0]
    tiles = rows // TILE
    q_rows = tab.shape[0] - 2 * W
    share = q_rows // n_sub
    s_rows = p16.shape[0]
    s_share = s_rows // n_sub
    k_q = qs_v.shape[0]
    k_s = cs_v.shape[0]
    send = Sends()

    def column_of(r):
        return lax.rem(x + r, n_x)

    def chip(r):
        return {"sub": 2 * lax.rem(x + r + n_x, n_x) + core}

    def patch(r):
        return {"patch": lax.rem(p + r + n_patch, n_patch)}

    def at(t, size):
        return pl.ds(pl.multiple_of(t * size, size), size)

    def load(src, dst, sem):
        c = pltpu.make_async_copy(src, dst, sem)
        c.start()
        return c

    load_nodes = load(nodes, nodes_v, load_sem.at[0])
    load_ei = load(edge_in, ei_v, load_sem.at[1])
    load_fs = load(f_senders, fs_v, load_sem.at[2])
    for i in range(tiles):
        load(f_edges.at[:, pl.ds(i * TILE, TILE), :], fe_v.at[i], edge_sem.at[i])
    load_rest = [
        load(edge_out, eo_v, load_sem.at[3]),
        load(node_in, ni_v, load_sem.at[4]),
        load(node_out, no_v, load_sem.at[5]),
    ]
    load_later = [
        load(q_edges.at[at(me, share * k_q), :], qe_v, load_sem.at[6]),
        load(q_senders, qs_v, load_sem.at[7]),
        load(c_edges, ce_v, load_sem.at[8]),
        load(c_senders.at[:, at(p, s_rows)], cs_v, load_sem.at[9]),
    ]

    after = {"patch": lax.rem(p + (me + 1) // n_sub, n_patch), "sub": lax.rem(me + 1, n_sub)}
    wrap = (n_sub - me) // n_sub
    before = {"patch": lax.rem(p + n_patch - wrap, n_patch), "sub": lax.rem(me + n_sub - 1, n_sub)}
    peers = [{"sub": lax.rem(me + r, n_sub)} for r in range(1, n_sub)]
    reached = [after, before] + peers + [patch(r) for r in (1, 2, -1, -2)]
    barrier = pltpu.get_barrier_semaphore()
    for to in reached:
        pl.semaphore_signal(barrier, inc=1, device_id=to, device_id_type=MESH)
    pool_rows = pool.shape[0]
    my_pool = pools.at[at(me, pool_rows), :]
    my_pool[...] = pool[...]

    load_nodes.wait()
    raw2 = split2(nodes_v[...])
    for k in range(2):
        fh_sent[k] = halves(dot(one_hot(column(f_halo[k : k + 1, :]), rows), raw2))
    pl.semaphore_wait(barrier, len(reached))
    fine_halo = [
        send(fh_sent.at[k], fh_got.at[k], fh_s.at[k], fh_r.at[k], to) for k, to in ((0, after), (1, before))
    ]
    pool_copies = [send(my_pool, my_pool, pl_s.at[r], pl_r.at[r], to) for r, to in enumerate(peers)]

    load_ei.wait()
    load_fs.wait()
    send_w = packed(ei_v[0, 0:W, :])
    recv_w = packed(ei_v[0, W : 2 * W, :])
    table[0:rows, :] = split2(halves(dot(raw2, send_w)))
    table[rows : rows + 2 * W, :] = packed(ei_v[0, 2 * W : 3 * W, :])

    def sender_columns(i):
        cols = []
        for k in range(degree):
            for j in range(TILE // W):
                cols.append(column(fs_v[k : k + 1, pl.ds(pl.multiple_of(i * TILE + j * W, W), W)]))
        return jnp.concatenate(cols, axis=0)

    def first_pass(i, carry):
        pltpu.make_async_copy(f_edges.at[:, pl.ds(0, TILE), :], fe_v.at[i], edge_sem.at[i]).wait()
        received = mm(nodes_v[at(i, TILE), :], recv_w)
        e2 = jnp.concatenate([split2(fe_v[i, k]) for k in range(degree)], axis=0)
        left = jnp.concatenate([one_hot(sender_columns(i), rows), e2], axis=1)
        zs[i] = halves(dot(left, table[0 : rows + 2 * W, :])) + jnp.concatenate([received] * degree, axis=0)
        return carry

    lax.fori_loop(0, tiles, first_pass, 0)
    for c in load_rest:
        c.wait()

    def level_weights(n):
        node_w = jnp.concatenate([packed(ni_v[n, 0:W, :]), packed(ni_v[n, W : 2 * W, :])], axis=0)
        return packed(centred_columns(eo_v[n])), node_w, packed(centred_columns(no_v[n]))

    out_w, node_w, last_w = level_weights(0)
    for c in fine_halo:
        c.wait_recv()
    halo_table = split2(mm(fh_got[...].reshape(2 * W, W), send_w))

    def second_pass(i, carry):
        hot = one_hot(sender_columns(i) - rows, 2 * W)
        hidden = jnp.maximum(zs[i] + halves(dot(hot, halo_table)), 0.0)
        message = scaled(mm(hidden, out_w))
        summed = fe_v[i, 0] + message[0:TILE]
        for k in range(1, degree):
            summed = summed + (fe_v[i, k] + message[k * TILE : (k + 1) * TILE])
        new = node_update(nodes_v[at(i, TILE), :], summed, node_w, last_w)
        new_v[at(i, TILE), :] = new
        news[at(i, TILE), :] = split2(new)
        return carry

    lax.fori_loop(0, tiles, second_pass, 0)

    def pair_sum(block, buf, ss, rs, r, size):
        return send(block.at[at(1 - core, size), :], buf.at[r], ss.at[r], rs.at[r], partner)

    pair = {}
    for r in (2, 1, 3, 0):
        first = pl.multiple_of(column_of(r) * 2 * share, 2 * share)
        sums_v[r] = halves(dot(one_hot_t(pool, first, 2 * share, pool_rows), news[...]))
        pair[r] = pair_sum(sums_v.at[r], pair_buf, pair_s, pair_r, r, share)
        if r == 1:
            pair[2].wait_recv()
            comb[2] = sums_v[2, at(core, share), :] + pair_buf[2]

    class RingSum:
        def __init__(self, part, stage, relay, arrive, ss, rs, half):
            self.part, self.stage, self.relay, self.arrive = part, stage, relay, arrive
            self.ss, self.rs, self.half = ss, rs, half

        def cut(self, r, h):
            return self.part.at[r, pl.ds(h * self.half, self.half), :]

        def far(self):
            self.relayed = [
                send(self.cut(2, h), self.relay.at[h], self.ss.at[h], self.rs.at[h], chip(1 - 2 * h)) for h in range(2)
            ]

        def near(self):
            self.plain = [
                send(self.cut(1 + 2 * h, 1 - h), self.arrive.at[h, 1 - h], self.ss.at[2 + h], self.rs.at[2 + h],
                     chip(1 - 2 * h))
                for h in range(2)
            ]

        def pass_on(self):
            self.joint = []
            for h in range(2):
                self.relayed[h].wait_recv()
                self.stage[h] = self.cut(1 + 2 * h, h)[...] + self.relay[h]
                self.joint.append(
                    send(self.stage.at[h], self.arrive.at[h, h], self.ss.at[4 + h], self.rs.at[4 + h], chip(1 - 2 * h))
                )

        def total(self):
            for c in self.plain + self.joint:
                c.wait_recv()
            return jnp.concatenate(
                [self.cut(0, h)[...] + self.arrive[0, h] + self.arrive[1, h] for h in range(2)], axis=0
            )

    sums = RingSum(comb, stage, relay_in, arrive, rs_s, rs_r, share // 2)
    sums.far()
    for r in (1, 3):
        pair[r].wait_recv()
        comb[r] = sums_v[r, at(core, share), :] + pair_buf[r]
    sums.near()
    pair[0].wait_recv()
    comb[0] = sums_v[0, at(core, share), :] + pair_buf[0]
    for c in load_later:
        c.wait()
    for k in range(k_q):
        row = qs_v[k : k + 1, at(me, share)]
        col = jnp.concatenate([column(row[:, j * W : (j + 1) * W]) for j in range(share // W)], axis=0)
        oh_q[k * share : (k + 1) * share, :] = one_hot(col, q_rows + 2 * W)
    sums.pass_on()
    for k in range(2):
        oh_h[k * W : (k + 1) * W, :] = one_hot(column(q_halo[k : k + 1, :]), q_rows)
    for c in pool_copies:
        c.wait_recv()
    counts = counts_of(pools, me * share, share, pools.shape[0])
    q_send_w = packed(ei_v[1, 0:W, :])
    q = sums.total() / counts
    tab[at(me, share), :] = mm(q, q_send_w)

    class RingGather:
        def __init__(self, buf, ss, rs, size):
            self.buf, self.ss, self.rs, self.size, self.half = buf, ss, rs, size, size // 2
            self.n, self.shared = 0, []
            self.from_near = {}
            for h in range(2):
                for way in range(2):
                    self.from_near[way, h ^ way] = self.go(0, h ^ way, chip(1 - 2 * way))
            for h in range(2):
                self.share_half(0, h)

        def cut(self, r, h):
            t = 2 * lax.rem(x + r + n_x, n_x) + core
            return self.buf.at[pl.ds(pl.multiple_of(t * self.size + h * self.half, self.half), self.half), :]

        def go(self, r, h, to):
            block = self.cut(r, h)
            c = send(block, block, self.ss.at[self.n], self.rs.at[self.n], to)
            self.n += 1
            return c

        def share_half(self, r, h):
            self.shared.append(self.go(r, h, partner))

        def pass_on(self):
            self.from_far = []
            for way in range(2):
                self.from_near[way, way].wait_recv()
                self.from_far.append(self.go(2 * way - 1, way, chip(1 - 2 * way)))
            for way in range(2):
                self.share_half(2 * way - 1, way)
            for way in range(2):
                self.from_near[way, 1 - way].wait_recv()
                self.share_half(2 * way - 1, 1 - way)

        def take_far(self):
            for way in range(2):
                self.from_far[way].wait_recv()
                self.share_half(2, way)

        def finish(self):
            for c in self.shared:
                c.wait_recv()

    around = RingGather(tab, ag_s, ag_r, share)
    q_recv = mm(q, packed(ei_v[1, W : 2 * W, :]))
    around.pass_on()
    edge_w = packed(ei_v[1, 2 * W : 3 * W, :])
    for k in range(k_q):
        base_v[k * share : (k + 1) * share, :] = mm(qe_v[pl.ds(k, share, stride=k_q), :], edge_w) + q_recv
    around.take_far()
    q_out_w, q_node_w, q_last_w = level_weights(1)
    own_pool = q_pool[pl.ds(me * (share // W), share // W), :]
    sub = sublanes(s_rows)
    hot16 = jnp.concatenate(
        [ones_where(jnp.broadcast_to(own_pool[j : j + 1, :], (s_rows, W)) == sub) for j in range(share // W)], axis=1
    )
    around.finish()
    table2 = split2(tab[0:q_rows, :])
    hsent[...] = halves(dot(oh_h[...], table2))
    halo = [
        send(hsent.at[pl.ds(k * W, W), :], tab.at[pl.ds(q_rows + k * W, W), :], h_s.at[k], h_r.at[k], patch(r))
        for k, r in ((0, 1), (1, -1))
    ]
    base = base_v[...] + halves(dot(oh_q[:, 0:q_rows], table2))
    for c in halo:
        c.wait_recv()
    halo2 = split2(tab[pl.ds(q_rows, 2 * W), :])
    hid = jnp.maximum(base + halves(dot(oh_q[:, q_rows : q_rows + 2 * W], halo2)), 0.0)
    msg = scaled(mm(hid, q_out_w))
    summed = None
    for k in range(k_q):
        term = qe_v[pl.ds(k, share, stride=k_q), :] + msg[k * share : (k + 1) * share]
        summed = term if summed is None else summed + term
    q_new = node_update(q, summed, q_node_w, q_last_w)
    qall[at(me, share), :] = q_new

    p16[...] = halves(dot(hot16, split2(q_new)))
    pair = {}
    for r in (2, 1, 3, 0):
        pair[r] = pair_sum(p16.at[at(column_of(r), 2 * s_share), :], pair16, pair16_s, pair16_r, r, s_share)
    sums = RingSum(comb16, stage16, relay16, arrive16, rs16_s, rs16_r, s_share // 2)
    for r in (2, 1, 3, 0):
        pair[r].wait_recv()
        t = 2 * column_of(r) + core
        comb16[r] = p16[at(t, s_share), :] + pair16[r]
        if r == 2:
            sums.far()
        if r == 3:
            sums.near()
    c_counts = counts_of(q_pool, me * s_share, s_share, q_pool.shape[0])
    c_send_w = packed(ei_v[2, 0:W, :])
    sums.pass_on()
    q_around = RingGather(qall, qg_s, qg_r, share)
    c_recv_w = packed(ei_v[2, W : 2 * W, :])
    c_edge_w = packed(ei_v[2, 2 * W : 3 * W, :])
    c = sums.total() / c_counts
    mine = pl.ds(pl.multiple_of(core * s_share, s_share), s_share)
    zt[p, mine, :] = mm(c, c_send_w)

    arrivals = {}

    def relay(src, sign, dist, last):
        block = zt.at[src, mine, :]
        way = 0 if sign > 0 else 1
        for hop in (2, 1):
            if dist + hop <= last:
                arrivals[sign, dist + hop] = send(
                    block, block, z_s.at[way, dist + hop], z_r.at[way, dist + hop], patch(sign * hop)
                )

    shared = []

    def hand_over(src, slot):
        block = zt.at[src, mine, :]
        shared.append(send(block, block, d_s.at[slot], d_r.at[slot], partner))

    far, near = n_patch // 2, n_patch - n_patch // 2 - 1
    limits = {1: far, -1: near}
    for sign in (1, -1):
        relay(p, sign, 0, limits[sign])
    hand_over(p, 0)

    def hot_pool():
        for j in range(rows // W):
            oh_p[j * W : (j + 1) * W, :] = one_hot(column(pool[j : j + 1, :]), q_rows)

    def hot_senders():
        for n, r in enumerate((2, 1, 3, 0)):
            for k in range(k_s):
                g = column(cs_v[k : k + 1, at(column_of(r), W)])
                g = jnp.where(core == 0, g[0:s_share], g[s_share : 2 * s_share])
                g = jnp.where((g // W) % n_x == x, (g // s_rows) * W + g % W, -1)
                first = n * k_s * s_share + k * s_share
                oh_c[first : first + s_share, :] = one_hot(g, n_patch * W)

    def hot_last():
        of_quarter = jnp.concatenate(
            [column(q_pool[j : j + 1, :]).astype(F32) for j in range(q_rows // W)], axis=0
        )
        target = halves(dot(oh_p[...], split2(of_quarter))).astype(jnp.int32)
        oh_t[...] = one_hot(target, s_rows)

    c_recv = mm(c, c_recv_w)
    c_base = []
    for k in range(k_s):
        c_base.append(mm(ce_v[pl.ds(k, s_share, stride=k_s), :], c_edge_w) + c_recv)

    def add_quarter():
        q_around.finish()
        new_v[...] = new_v[...] + halves(dot(oh_p[...], split2(qall[...])))

    between = {2: [q_around.pass_on, hot_senders], 4: [q_around.take_far, hot_pool], 6: [hot_last], 8: []}
    for dist in range(2, far + 2, 2):
        for work in between.get(dist, []):
            work()
        for d in (dist, dist - 1):
            for sign in (1, -1):
                if d <= limits[sign]:
                    arrivals[sign, d].wait_recv()
                    src = lax.rem(p - sign * d + n_patch, n_patch)
                    if d == dist:
                        relay(src, sign, d, limits[sign])
                    hand_over(src, d if sign > 0 else far + d)
    c_out_w, c_node_w, c_last_w = level_weights(2)
    for s in shared:
        s.wait_recv()
    ztable = split2(zt[...].reshape(n_patch * 2 * s_share, W))
    size = k_s * s_share
    sums = RingSum(gpart, gstage, grelay, garrive, g_s, g_r, size // 2)
    for n, r in enumerate((2, 1, 3, 0)):
        gpart[r] = halves(dot(oh_c[n * size : (n + 1) * size, :], ztable))
        if r == 2:
            sums.far()
        if r == 3:
            sums.near()
    sums.pass_on()
    add_quarter()
    hid = jnp.maximum(jnp.concatenate(c_base, axis=0) + sums.total(), 0.0)
    msg = scaled(mm(hid, c_out_w))
    summed = None
    for k in range(k_s):
        term = ce_v[pl.ds(k, s_share, stride=k_s), :] + msg[k * s_share : (k + 1) * s_share]
        summed = term if summed is None else summed + term
    ctab[at(me, s_share), :] = node_update(c, summed, c_node_w, c_last_w)
    c_around = RingGather(ctab, cg_s, cg_r, s_share)
    c_around.pass_on()
    c_around.take_far()
    c_around.finish()
    out[...] = new_v[...] + halves(dot(oh_t[...], split2(ctab[...])))
    for s in send.all:
        s.wait_send()


def all_levels(n_patch, n_sub, nodes, f_edges, f_senders, f_halo, pool, q_edges, q_senders, q_halo, q_pool, c_edges,
               c_senders, edge_in, edge_out, node_in, node_out):
    any_ = pl.BlockSpec(memory_space=pl.ANY)
    vm = pl.BlockSpec(memory_space=pltpu.VMEM)
    degree, rows, _ = f_edges.shape
    k_q, q_rows = q_senders.shape
    share = q_rows // n_sub
    k_s = c_senders.shape[0]
    s_rows = c_senders.shape[1] // n_patch
    s_share = s_rows // n_sub
    n_x = n_sub // 2
    dma = pltpu.SemaphoreType.DMA
    v = lambda *shape: pltpu.VMEM(shape, F32)
    b = lambda *shape: pltpu.VMEM(shape, BF)
    i32 = lambda *shape: pltpu.VMEM(shape, jnp.int32)
    gsems = [dma((14,)), dma((14,))]
    return pl.pallas_call(
        functools.partial(levels_kernel, n_patch, n_sub),
        name="all_levels",
        out_shape=jax.ShapeDtypeStruct((rows, W), F32),
        in_specs=[any_, any_, any_, vm, vm, any_, any_, vm, vm, any_, any_, any_, any_, any_, any_],
        out_specs=vm,
        scratch_shapes=[
            v(rows, W), v(rows // TILE, degree, TILE, W), i32(degree, rows),
            v(share * k_q, W), i32(k_q, q_rows), v(s_share * k_s, W), i32(k_s, s_rows),
            v(*edge_in.shape), v(*edge_out.shape), v(*node_in.shape), v(*node_out.shape),
            i32(n_sub * pool.shape[0], W), v(2, W, W), v(2, W, W),
            b(rows + 2 * W, 2 * W), b(rows, 2 * W), v(rows // TILE, degree * TILE, W), v(rows, W),
            v(n_x, 2 * share, W), v(n_x, share, W), v(n_x, share, W),
            v(2, share // 2, W), v(2, share // 2, W), v(2, 2, share // 2, W),
            v(q_rows + 2 * W, W), v(2 * W, W), v(q_rows, W),
            b(k_q * share, q_rows + 2 * W), b(2 * W, q_rows), b(n_x * k_s * s_share, n_patch * W),
            b(rows, q_rows), b(rows, s_rows), v(k_q * share, W),
            v(s_rows, W), v(n_x, s_share, W), v(n_x, s_share, W),
            v(2, s_share // 2, W), v(2, s_share // 2, W), v(2, 2, s_share // 2, W),
            v(n_patch, 2 * s_share, W), v(n_x, k_s * s_share, W),
            v(2, k_s * s_share // 2, W), v(2, k_s * s_share // 2, W), v(2, 2, k_s * s_share // 2, W), v(s_rows, W),
            dma((10,)), dma((rows // TILE,)), dma((2,)), dma((2,)), dma((n_sub - 1,)), dma((n_sub - 1,)),
            dma((n_x,)), dma((n_x,)), dma((6,)), dma((6,)), *gsems, dma((2,)), dma((2,)),
            dma((n_x,)), dma((n_x,)), dma((6,)), dma((6,)), *gsems,
            dma((2, n_patch)), dma((2, n_patch)), dma((n_patch,)), dma((n_patch,)),
            dma((6,)), dma((6,)), *gsems,
        ],
        compiler_params=pltpu.CompilerParams(collective_id=0, has_side_effects=True, vmem_limit_bytes=VMEM_LIMIT),
    )(nodes, f_edges, f_senders, f_halo, pool, q_edges, q_senders, q_halo, q_pool, c_edges, c_senders, edge_in,
      edge_out, node_in, node_out)


def on_device(n_patch, n_sub, fine_nodes, fine_edges, fine_senders, fine_halo, fine_pool, quarter_edges,
              quarter_senders, quarter_halo, quarter_pool, coarse_edges, coarse_senders, edge_in, edge_out, node_in,
              node_out):
    return all_levels(n_patch, n_sub, fine_nodes, fine_edges.transpose(1, 0, 2), fine_senders.T, fine_halo,
                      fine_pool.reshape(-1, W), quarter_edges.reshape(-1, W), quarter_senders.T, quarter_halo,
                      quarter_pool.reshape(-1, W), coarse_edges.reshape(-1, W), coarse_senders.T, edge_in, edge_out,
                      node_in, node_out)


def solution(mesh):
    both = ("groups", "patch", "sub")
    halfway = ("groups", "patch")
    in_specs = (
        P(both, None),
        P(both, None, None),
        P(both, None),
        P(both, None),
        P(both),
        P(halfway, None, None),
        P(halfway, None),
        P(halfway, None),
        P(halfway),
        P(both, None, None),
        P("groups", None),
        P(),
        P(),
        P(),
        P(),
    )
    return jax.shard_map(
        functools.partial(on_device, mesh.shape["patch"], mesh.shape["sub"]),
        mesh=mesh,
        in_specs=in_specs,
        out_specs=P(both, None),
        check_vma=False,
    )
```

```python
import functools

import jax
import jax.numpy as jnp
from jax import lax
from jax.experimental import pallas as pl
from jax.experimental.pallas import tpu as pltpu
from jax.sharding import PartitionSpec as P

MESH = pl.DeviceIdType.MESH
BF = jnp.bfloat16
F32 = jnp.float32
W = 128
VMEM_LIMIT = 56 * 1024 * 1024


def split2(x):
    hi = x.astype(BF)
    lo = (x - hi.astype(F32)).astype(BF)
    return jnp.concatenate([hi, lo], axis=1)


def packed(w):
    s = split2(w)
    return jnp.concatenate([s, s], axis=0)


def halves(y):
    return y[:, :W] + y[:, W:]


def dot(a, b):
    return jnp.dot(a, b, preferred_element_type=F32)


def mm(x, wp):
    return halves(dot(split2(x), wp))


def centred_columns(w):
    return w - jnp.mean(w, axis=1, keepdims=True)


def scaled(m):
    return m * lax.rsqrt(jnp.mean(m * m, axis=1, keepdims=True) + 1e-05)


def column(row):
    return jnp.broadcast_to(row, (W, W)).T


def lanes(rows):
    return lax.broadcasted_iota(jnp.int32, (rows, W), 1)


def sublanes(rows):
    return lax.broadcasted_iota(jnp.int32, (rows, W), 0)


def ones_where(mask):
    return jnp.where(mask, 1.0, 0.0).astype(BF)


def one_hot(col, width):
    lane = lanes(col.shape[0])
    return jnp.concatenate([ones_where(col == lane + j * W) for j in range(width // W)], axis=1)


def one_hot_t(index_ref, first, rows, blocks):
    sub = sublanes(rows) + first
    return jnp.concatenate(
        [ones_where(jnp.broadcast_to(index_ref[j : j + 1, :], (rows, W)) == sub) for j in range(blocks)],
        axis=1,
    )


def counts_of(index_ref, first, rows, blocks):
    sub = sublanes(rows) + first

    def add(j, acc):
        row = jnp.broadcast_to(index_ref[pl.ds(j, 1), :], (rows, W))
        return acc + jnp.where(row == sub, 1.0, 0.0)

    acc = lax.fori_loop(0, blocks, add, jnp.zeros((rows, W), F32))
    return jnp.sum(acc, axis=1, keepdims=True)


TILE = 512


class Sends:
    def __init__(self):
        self.all = []

    def __call__(self, src, dst, ss, rs, to):
        c = pltpu.make_async_remote_copy(src, dst, ss, rs, device_id=to, device_id_type=MESH)
        c.start()
        self.all.append(c)
        return c


def node_update(h, summed, node_w, last_w):
    both = jnp.concatenate([split2(h), split2(summed)], axis=1)
    a = jnp.maximum(halves(dot(both, node_w)), 0.0)
    return h + scaled(mm(a, last_w))


def levels_kernel(n_patch, n_sub,
                  nodes, f_edges, f_senders, f_halo, pool, q_edges, q_senders, q_halo, q_pool, c_edges, c_senders,
                  edge_in, edge_out, node_in, node_out,
                  out,
                  nodes_v, fe_v, fs_v, qe_v, qs_v, ce_v, cs_v, ei_v, eo_v, ni_v, no_v,
                  pools, fh_sent, fh_got, table, news, zs, new_v,
                  sums_v, pair_buf, comb, stage, relay_in, arrive,
                  tab, hsent, qall, oh_q, oh_h, oh_c, oh_p, oh_t, base_v,
                  p16, pair16, comb16, stage16, relay16, arrive16, zt, gpart, gstage, grelay, garrive, ctab,
                  load_sem, edge_sem, fh_s, fh_r, pl_s, pl_r,
                  pair_s, pair_r, rs_s, rs_r, ag_s, ag_r, h_s, h_r,
                  pair16_s, pair16_r, rs16_s, rs16_r, qg_s, qg_r, z_s, z_r, d_s, d_r, g_s, g_r, cg_s, cg_r):
    p, me = lax.axis_index("patch"), lax.axis_index("sub")
    core = lax.rem(me, 2)
    x = me // 2
    n_x = n_sub // 2
    partner = {"sub": me + 1 - 2 * core}
    rows = nodes.shape[0]
    degree = f_edges.shape[0]
    tiles = rows // TILE
    q_rows = tab.shape[0] - 2 * W
    share = q_rows // n_sub
    s_rows = p16.shape[0]
    s_share = s_rows // n_sub
    k_q = qs_v.shape[0]
    k_s = cs_v.shape[0]
    send = Sends()

    def column_of(r):
        return lax.rem(x + r, n_x)

    def chip(r):
        return {"sub": 2 * lax.rem(x + r + n_x, n_x) + core}

    def patch(r):
        return {"patch": lax.rem(p + r + n_patch, n_patch)}

    def at(t, size):
        return pl.ds(pl.multiple_of(t * size, size), size)

    def load(src, dst, sem):
        c = pltpu.make_async_copy(src, dst, sem)
        c.start()
        return c

    load_nodes = load(nodes, nodes_v, load_sem.at[0])
    load_ei = load(edge_in, ei_v, load_sem.at[1])
    load_fs = load(f_senders, fs_v, load_sem.at[2])
    for i in range(tiles):
        load(f_edges.at[:, pl.ds(i * TILE, TILE), :], fe_v.at[i], edge_sem.at[i])
    load_rest = [
        load(edge_out, eo_v, load_sem.at[3]),
        load(node_in, ni_v, load_sem.at[4]),
        load(node_out, no_v, load_sem.at[5]),
    ]
    load_later = [
        load(q_edges.at[at(me, share * k_q), :], qe_v, load_sem.at[6]),
        load(q_senders, qs_v, load_sem.at[7]),
        load(c_edges, ce_v, load_sem.at[8]),
        load(c_senders.at[:, at(p, s_rows)], cs_v, load_sem.at[9]),
    ]

    after = {"patch": lax.rem(p + (me + 1) // n_sub, n_patch), "sub": lax.rem(me + 1, n_sub)}
    wrap = (n_sub - me) // n_sub
    before = {"patch": lax.rem(p + n_patch - wrap, n_patch), "sub": lax.rem(me + n_sub - 1, n_sub)}
    peers = [{"sub": lax.rem(me + r, n_sub)} for r in range(1, n_sub)]
    reached = [after, before] + peers + [patch(r) for r in (1, 2, -1, -2)]
    barrier = pltpu.get_barrier_semaphore()
    for to in reached:
        pl.semaphore_signal(barrier, inc=1, device_id=to, device_id_type=MESH)
    pool_rows = pool.shape[0]
    my_pool = pools.at[at(me, pool_rows), :]
    my_pool[...] = pool[...]

    load_nodes.wait()
    raw2 = split2(nodes_v[...])
    for k in range(2):
        fh_sent[k] = halves(dot(one_hot(column(f_halo[k : k + 1, :]), rows), raw2))
    pl.semaphore_wait(barrier, len(reached))
    fine_halo = [
        send(fh_sent.at[k], fh_got.at[k], fh_s.at[k], fh_r.at[k], to) for k, to in ((0, after), (1, before))
    ]
    pool_copies = [send(my_pool, my_pool, pl_s.at[r], pl_r.at[r], to) for r, to in enumerate(peers)]

    load_ei.wait()
    load_fs.wait()
    send_w = packed(ei_v[0, 0:W, :])
    recv_w = packed(ei_v[0, W : 2 * W, :])
    table[0:rows, :] = split2(halves(dot(raw2, send_w)))
    table[rows : rows + 2 * W, :] = packed(ei_v[0, 2 * W : 3 * W, :])

    def sender_columns(i):
        cols = []
        for k in range(degree):
            for j in range(TILE // W):
                cols.append(column(fs_v[k : k + 1, pl.ds(pl.multiple_of(i * TILE + j * W, W), W)]))
        return jnp.concatenate(cols, axis=0)

    def first_pass(i, carry):
        pltpu.make_async_copy(f_edges.at[:, pl.ds(0, TILE), :], fe_v.at[i], edge_sem.at[i]).wait()
        received = mm(nodes_v[at(i, TILE), :], recv_w)
        e2 = jnp.concatenate([split2(fe_v[i, k]) for k in range(degree)], axis=0)
        left = jnp.concatenate([one_hot(sender_columns(i), rows), e2], axis=1)
        zs[i] = halves(dot(left, table[0 : rows + 2 * W, :])) + jnp.concatenate([received] * degree, axis=0)
        return carry

    lax.fori_loop(0, tiles, first_pass, 0)
    for c in load_rest:
        c.wait()

    def level_weights(n):
        node_w = jnp.concatenate([packed(ni_v[n, 0:W, :]), packed(ni_v[n, W : 2 * W, :])], axis=0)
        return packed(centred_columns(eo_v[n])), node_w, packed(centred_columns(no_v[n]))

    out_w, node_w, last_w = level_weights(0)
    for c in fine_halo:
        c.wait_recv()
    halo_table = split2(mm(fh_got[...].reshape(2 * W, W), send_w))

    def second_pass(i, carry):
        hot = one_hot(sender_columns(i) - rows, 2 * W)
        hidden = jnp.maximum(zs[i] + halves(dot(hot, halo_table)), 0.0)
        message = scaled(mm(hidden, out_w))
        summed = fe_v[i, 0] + message[0:TILE]
        for k in range(1, degree):
            summed = summed + (fe_v[i, k] + message[k * TILE : (k + 1) * TILE])
        new = node_update(nodes_v[at(i, TILE), :], summed, node_w, last_w)
        new_v[at(i, TILE), :] = new
        news[at(i, TILE), :] = split2(new)
        return carry

    lax.fori_loop(0, tiles, second_pass, 0)

    class RingSum:
        def __init__(self, part, stage, relay, arrive, ss, rs, half):
            self.part, self.stage, self.relay, self.arrive = part, stage, relay, arrive
            self.ss, self.rs, self.half = ss, rs, half

        def cut(self, r, h):
            return self.part.at[r, pl.ds(h * self.half, self.half), :]

        def far(self):
            self.relayed = [
                send(self.cut(2, h), self.relay.at[h], self.ss.at[h], self.rs.at[h], chip(1 - 2 * h)) for h in range(2)
            ]

        def near(self):
            self.plain = [
                send(self.cut(1 + 2 * h, 1 - h), self.arrive.at[h, 1 - h], self.ss.at[2 + h], self.rs.at[2 + h],
                     chip(1 - 2 * h))
                for h in range(2)
            ]

        def pass_on(self):
            self.joint = []
            for h in range(2):
                self.relayed[h].wait_recv()
                self.stage[h] = self.cut(1 + 2 * h, h)[...] + self.relay[h]
                self.joint.append(
                    send(self.stage.at[h], self.arrive.at[h, h], self.ss.at[4 + h], self.rs.at[4 + h], chip(1 - 2 * h))
                )

        def total(self):
            for c in self.plain + self.joint:
                c.wait_recv()
            return jnp.concatenate(
                [self.cut(0, h)[...] + self.arrive[0, h] + self.arrive[1, h] for h in range(2)], axis=0
            )

    def hot_pool():
        for j in range(rows // W):
            oh_p[j * W : (j + 1) * W, :] = one_hot(column(pool[j : j + 1, :]), q_rows)

    def hot_senders():
        for n, r in enumerate((2, 1, 3, 0)):
            for k in range(k_s):
                g = column(cs_v[k : k + 1, at(column_of(r), W)])
                g = jnp.where(core == 0, g[0:s_share], g[s_share : 2 * s_share])
                g = jnp.where((g // W) % n_x == x, (g // s_rows) * W + g % W, -1)
                first = n * k_s * s_share + k * s_share
                oh_c[first : first + s_share, :] = one_hot(g, n_patch * W)

    def hot_last():
        of_quarter = jnp.concatenate(
            [column(q_pool[j : j + 1, :]).astype(F32) for j in range(q_rows // W)], axis=0
        )
        target = halves(dot(oh_p[...], split2(of_quarter))).astype(jnp.int32)
        oh_t[...] = one_hot(target, s_rows)

    def pair_sum(block, buf, ss, rs, r, size):
        return send(block.at[at(1 - core, size), :], buf.at[r], ss.at[r], rs.at[r], partner)

    pair = {}
    sums = RingSum(comb, stage, relay_in, arrive, rs_s, rs_r, share // 2)
    for r in (2, 1, 3, 0):
        first = pl.multiple_of(column_of(r) * 2 * share, 2 * share)
        sums_v[r] = halves(dot(one_hot_t(pool, first, 2 * share, pool_rows), news[...]))
        pair[r] = pair_sum(sums_v.at[r], pair_buf, pair_s, pair_r, r, share)
        if r == 1:
            pair[2].wait_recv()
            comb[2] = sums_v[2, at(core, share), :] + pair_buf[2]
            sums.far()

    for r in (1, 3):
        pair[r].wait_recv()
        comb[r] = sums_v[r, at(core, share), :] + pair_buf[r]
    sums.near()
    pair[0].wait_recv()
    comb[0] = sums_v[0, at(core, share), :] + pair_buf[0]
    for c in load_later:
        c.wait()
    for k in range(k_q):
        row = qs_v[k : k + 1, at(me, share)]
        col = jnp.concatenate([column(row[:, j * W : (j + 1) * W]) for j in range(share // W)], axis=0)
        oh_q[k * share : (k + 1) * share, :] = one_hot(col, q_rows + 2 * W)
    sums.pass_on()
    for k in range(2):
        oh_h[k * W : (k + 1) * W, :] = one_hot(column(q_halo[k : k + 1, :]), q_rows)
    for c in pool_copies:
        c.wait_recv()
    counts = counts_of(pools, me * share, share, pools.shape[0])
    hot_pool()
    q_send_w = packed(ei_v[1, 0:W, :])
    q = sums.total() / counts
    tab[at(me, share), :] = mm(q, q_send_w)

    class RingGather:
        def __init__(self, buf, ss, rs, size):
            self.buf, self.ss, self.rs, self.size, self.half = buf, ss, rs, size, size // 2
            self.n, self.shared = 0, []
            self.from_near = {}
            for h in range(2):
                for way in range(2):
                    self.from_near[way, h ^ way] = self.go(0, h ^ way, chip(1 - 2 * way))
            for h in range(2):
                self.share_half(0, h)

        def cut(self, r, h):
            t = 2 * lax.rem(x + r + n_x, n_x) + core
            return self.buf.at[pl.ds(pl.multiple_of(t * self.size + h * self.half, self.half), self.half), :]

        def go(self, r, h, to):
            block = self.cut(r, h)
            c = send(block, block, self.ss.at[self.n], self.rs.at[self.n], to)
            self.n += 1
            return c

        def share_half(self, r, h):
            self.shared.append(self.go(r, h, partner))

        def pass_on(self):
            self.from_far = []
            for way in range(2):
                self.from_near[way, way].wait_recv()
                self.from_far.append(self.go(2 * way - 1, way, chip(1 - 2 * way)))
            for way in range(2):
                self.share_half(2 * way - 1, way)
            for way in range(2):
                self.from_near[way, 1 - way].wait_recv()
                self.share_half(2 * way - 1, 1 - way)

        def take_far(self):
            for way in range(2):
                self.from_far[way].wait_recv()
                self.share_half(2, way)

        def finish(self):
            for c in self.shared:
                c.wait_recv()

    around = RingGather(tab, ag_s, ag_r, share)
    q_recv = mm(q, packed(ei_v[1, W : 2 * W, :]))
    hot_senders()
    around.pass_on()
    edge_w = packed(ei_v[1, 2 * W : 3 * W, :])
    for k in range(k_q):
        base_v[k * share : (k + 1) * share, :] = mm(qe_v[pl.ds(k, share, stride=k_q), :], edge_w) + q_recv
    around.take_far()
    q_out_w, q_node_w, q_last_w = level_weights(1)
    own_pool = q_pool[pl.ds(me * (share // W), share // W), :]
    sub = sublanes(s_rows)
    hot16 = jnp.concatenate(
        [ones_where(jnp.broadcast_to(own_pool[j : j + 1, :], (s_rows, W)) == sub) for j in range(share // W)], axis=1
    )
    around.finish()
    table2 = split2(tab[0:q_rows, :])
    hsent[...] = halves(dot(oh_h[...], table2))
    halo = [
        send(hsent.at[pl.ds(k * W, W), :], tab.at[pl.ds(q_rows + k * W, W), :], h_s.at[k], h_r.at[k], patch(r))
        for k, r in ((0, 1), (1, -1))
    ]
    base = base_v[...] + halves(dot(oh_q[:, 0:q_rows], table2))
    hot_last()
    for c in halo:
        c.wait_recv()
    halo2 = split2(tab[pl.ds(q_rows, 2 * W), :])
    hid = jnp.maximum(base + halves(dot(oh_q[:, q_rows : q_rows + 2 * W], halo2)), 0.0)
    msg = scaled(mm(hid, q_out_w))
    summed = None
    for k in range(k_q):
        term = qe_v[pl.ds(k, share, stride=k_q), :] + msg[k * share : (k + 1) * share]
        summed = term if summed is None else summed + term
    q_new = node_update(q, summed, q_node_w, q_last_w)
    qall[at(me, share), :] = q_new

    p16[...] = halves(dot(hot16, split2(q_new)))
    pair = {}
    for r in (2, 1, 3, 0):
        pair[r] = pair_sum(p16.at[at(column_of(r), 2 * s_share), :], pair16, pair16_s, pair16_r, r, s_share)
    sums = RingSum(comb16, stage16, relay16, arrive16, rs16_s, rs16_r, s_share // 2)
    for r in (2, 1, 3, 0):
        pair[r].wait_recv()
        t = 2 * column_of(r) + core
        comb16[r] = p16[at(t, s_share), :] + pair16[r]
        if r == 2:
            sums.far()
        if r == 3:
            sums.near()
    c_counts = counts_of(q_pool, me * s_share, s_share, q_pool.shape[0])
    c_send_w = packed(ei_v[2, 0:W, :])
    sums.pass_on()
    q_around = RingGather(qall, qg_s, qg_r, share)
    c_recv_w = packed(ei_v[2, W : 2 * W, :])
    c_edge_w = packed(ei_v[2, 2 * W : 3 * W, :])
    c = sums.total() / c_counts
    mine = pl.ds(pl.multiple_of(core * s_share, s_share), s_share)
    zt[p, mine, :] = mm(c, c_send_w)

    arrivals = {}

    def relay(src, sign, dist, last):
        block = zt.at[src, mine, :]
        way = 0 if sign > 0 else 1
        for hop in (2, 1):
            if dist + hop <= last:
                arrivals[sign, dist + hop] = send(
                    block, block, z_s.at[way, dist + hop], z_r.at[way, dist + hop], patch(sign * hop)
                )

    shared = []

    def hand_over(src, slot):
        block = zt.at[src, mine, :]
        shared.append(send(block, block, d_s.at[slot], d_r.at[slot], partner))

    far, near = n_patch // 2, n_patch - n_patch // 2 - 1
    limits = {1: far, -1: near}
    for sign in (1, -1):
        relay(p, sign, 0, limits[sign])
    hand_over(p, 0)

    c_recv = mm(c, c_recv_w)
    c_base = []
    for k in range(k_s):
        c_base.append(mm(ce_v[pl.ds(k, s_share, stride=k_s), :], c_edge_w) + c_recv)

    def add_quarter():
        q_around.finish()
        new_v[...] = new_v[...] + halves(dot(oh_p[...], split2(qall[...])))

    between = {2: q_around.pass_on, 4: q_around.take_far}
    for dist in range(2, far + 2, 2):
        for d in (dist, dist - 1):
            for sign in (1, -1):
                if d <= limits[sign]:
                    arrivals[sign, d].wait_recv()
                    src = lax.rem(p - sign * d + n_patch, n_patch)
                    if d == dist:
                        relay(src, sign, d, limits[sign])
                    hand_over(src, d if sign > 0 else far + d)
        if dist in between:
            between[dist]()
    c_out_w, c_node_w, c_last_w = level_weights(2)
    for s in shared:
        s.wait_recv()
    ztable = split2(zt[...].reshape(n_patch * 2 * s_share, W))
    size = k_s * s_share
    sums = RingSum(gpart, gstage, grelay, garrive, g_s, g_r, size // 2)
    for n, r in enumerate((2, 1, 3, 0)):
        gpart[r] = halves(dot(oh_c[n * size : (n + 1) * size, :], ztable))
        if r == 2:
            sums.far()
        if r == 3:
            sums.near()
    sums.pass_on()
    add_quarter()
    hid = jnp.maximum(jnp.concatenate(c_base, axis=0) + sums.total(), 0.0)
    msg = scaled(mm(hid, c_out_w))
    summed = None
    for k in range(k_s):
        term = ce_v[pl.ds(k, s_share, stride=k_s), :] + msg[k * s_share : (k + 1) * s_share]
        summed = term if summed is None else summed + term
    ctab[at(me, s_share), :] = node_update(c, summed, c_node_w, c_last_w)
    c_around = RingGather(ctab, cg_s, cg_r, s_share)
    c_around.pass_on()
    c_around.take_far()
    c_around.finish()
    out[...] = new_v[...] + halves(dot(oh_t[...], split2(ctab[...])))
    for s in send.all:
        s.wait_send()


def all_levels(n_patch, n_sub, nodes, f_edges, f_senders, f_halo, pool, q_edges, q_senders, q_halo, q_pool, c_edges,
               c_senders, edge_in, edge_out, node_in, node_out):
    any_ = pl.BlockSpec(memory_space=pl.ANY)
    vm = pl.BlockSpec(memory_space=pltpu.VMEM)
    degree, rows, _ = f_edges.shape
    k_q, q_rows = q_senders.shape
    share = q_rows // n_sub
    k_s = c_senders.shape[0]
    s_rows = c_senders.shape[1] // n_patch
    s_share = s_rows // n_sub
    n_x = n_sub // 2
    dma = pltpu.SemaphoreType.DMA
    v = lambda *shape: pltpu.VMEM(shape, F32)
    b = lambda *shape: pltpu.VMEM(shape, BF)
    i32 = lambda *shape: pltpu.VMEM(shape, jnp.int32)
    gsems = [dma((14,)), dma((14,))]
    return pl.pallas_call(
        functools.partial(levels_kernel, n_patch, n_sub),
        name="all_levels",
        out_shape=jax.ShapeDtypeStruct((rows, W), F32),
        in_specs=[any_, any_, any_, vm, vm, any_, any_, vm, vm, any_, any_, any_, any_, any_, any_],
        out_specs=vm,
        scratch_shapes=[
            v(rows, W), v(rows // TILE, degree, TILE, W), i32(degree, rows),
            v(share * k_q, W), i32(k_q, q_rows), v(s_share * k_s, W), i32(k_s, s_rows),
            v(*edge_in.shape), v(*edge_out.shape), v(*node_in.shape), v(*node_out.shape),
            i32(n_sub * pool.shape[0], W), v(2, W, W), v(2, W, W),
            b(rows + 2 * W, 2 * W), b(rows, 2 * W), v(rows // TILE, degree * TILE, W), v(rows, W),
            v(n_x, 2 * share, W), v(n_x, share, W), v(n_x, share, W),
            v(2, share // 2, W), v(2, share // 2, W), v(2, 2, share // 2, W),
            v(q_rows + 2 * W, W), v(2 * W, W), v(q_rows, W),
            b(k_q * share, q_rows + 2 * W), b(2 * W, q_rows), b(n_x * k_s * s_share, n_patch * W),
            b(rows, q_rows), b(rows, s_rows), v(k_q * share, W),
            v(s_rows, W), v(n_x, s_share, W), v(n_x, s_share, W),
            v(2, s_share // 2, W), v(2, s_share // 2, W), v(2, 2, s_share // 2, W),
            v(n_patch, 2 * s_share, W), v(n_x, k_s * s_share, W),
            v(2, k_s * s_share // 2, W), v(2, k_s * s_share // 2, W), v(2, 2, k_s * s_share // 2, W), v(s_rows, W),
            dma((10,)), dma((rows // TILE,)), dma((2,)), dma((2,)), dma((n_sub - 1,)), dma((n_sub - 1,)),
            dma((n_x,)), dma((n_x,)), dma((6,)), dma((6,)), *gsems, dma((2,)), dma((2,)),
            dma((n_x,)), dma((n_x,)), dma((6,)), dma((6,)), *gsems,
            dma((2, n_patch)), dma((2, n_patch)), dma((n_patch,)), dma((n_patch,)),
            dma((6,)), dma((6,)), *gsems,
        ],
        compiler_params=pltpu.CompilerParams(collective_id=0, has_side_effects=True, vmem_limit_bytes=VMEM_LIMIT),
    )(nodes, f_edges, f_senders, f_halo, pool, q_edges, q_senders, q_halo, q_pool, c_edges, c_senders, edge_in,
      edge_out, node_in, node_out)


def on_device(n_patch, n_sub, fine_nodes, fine_edges, fine_senders, fine_halo, fine_pool, quarter_edges,
              quarter_senders, quarter_halo, quarter_pool, coarse_edges, coarse_senders, edge_in, edge_out, node_in,
              node_out):
    return all_levels(n_patch, n_sub, fine_nodes, fine_edges.transpose(1, 0, 2), fine_senders.T, fine_halo,
                      fine_pool.reshape(-1, W), quarter_edges.reshape(-1, W), quarter_senders.T, quarter_halo,
                      quarter_pool.reshape(-1, W), coarse_edges.reshape(-1, W), coarse_senders.T, edge_in, edge_out,
                      node_in, node_out)


def solution(mesh):
    both = ("groups", "patch", "sub")
    halfway = ("groups", "patch")
    in_specs = (
        P(both, None),
        P(both, None, None),
        P(both, None),
        P(both, None),
        P(both),
        P(halfway, None, None),
        P(halfway, None),
        P(halfway, None),
        P(halfway),
        P(both, None, None),
        P("groups", None),
        P(),
        P(),
        P(),
        P(),
    )
    return jax.shard_map(
        functools.partial(on_device, mesh.shape["patch"], mesh.shape["sub"]),
        mesh=mesh,
        in_specs=in_specs,
        out_specs=P(both, None),
        check_vma=False,
    )
```

```python
import functools

import jax
import jax.numpy as jnp
from jax import lax
from jax.experimental import pallas as pl
from jax.experimental.pallas import tpu as pltpu
from jax.sharding import PartitionSpec as P

MESH = pl.DeviceIdType.MESH
BF = jnp.bfloat16
F32 = jnp.float32
W = 128
VMEM_LIMIT = 56 * 1024 * 1024


def split2(x):
    hi = x.astype(BF)
    lo = (x - hi.astype(F32)).astype(BF)
    return jnp.concatenate([hi, lo], axis=1)


def packed(w):
    s = split2(w)
    return jnp.concatenate([s, s], axis=0)


def halves(y):
    return y[:, :W] + y[:, W:]


def dot(a, b):
    return jnp.dot(a, b, preferred_element_type=F32)


def mm(x, wp):
    return halves(dot(split2(x), wp))


def centred_columns(w):
    return w - jnp.mean(w, axis=1, keepdims=True)


def scaled(m):
    return m * lax.rsqrt(jnp.mean(m * m, axis=1, keepdims=True) + 1e-05)


def column(row):
    return jnp.broadcast_to(row, (W, W)).T


def lanes(rows):
    return lax.broadcasted_iota(jnp.int32, (rows, W), 1)


def sublanes(rows):
    return lax.broadcasted_iota(jnp.int32, (rows, W), 0)


def ones_where(mask):
    return jnp.where(mask, 1.0, 0.0).astype(BF)


def one_hot(col, width):
    lane = lanes(col.shape[0])
    return jnp.concatenate([ones_where(col == lane + j * W) for j in range(width // W)], axis=1)


def one_hot_t(index_ref, first, rows, blocks):
    sub = sublanes(rows) + first
    return jnp.concatenate(
        [ones_where(jnp.broadcast_to(index_ref[j : j + 1, :], (rows, W)) == sub) for j in range(blocks)],
        axis=1,
    )


def counts_of(index_ref, first, rows, blocks):
    sub = sublanes(rows) + first

    def add(j, acc):
        row = jnp.broadcast_to(index_ref[pl.ds(j, 1), :], (rows, W))
        return acc + jnp.where(row == sub, 1.0, 0.0)

    acc = lax.fori_loop(0, blocks, add, jnp.zeros((rows, W), F32))
    return jnp.sum(acc, axis=1, keepdims=True)


TILE = 512


class Sends:
    def __init__(self):
        self.all = []

    def __call__(self, src, dst, ss, rs, to):
        c = pltpu.make_async_remote_copy(src, dst, ss, rs, device_id=to, device_id_type=MESH)
        c.start()
        self.all.append(c)
        return c


def node_update(h, summed, node_w, last_w):
    both = jnp.concatenate([split2(h), split2(summed)], axis=1)
    a = jnp.maximum(halves(dot(both, node_w)), 0.0)
    return h + scaled(mm(a, last_w))


def levels_kernel(n_patch, n_sub,
                  nodes, f_edges, f_senders, f_halo, pool, q_edges, q_senders, q_halo, q_pool, c_edges, c_senders,
                  edge_in, edge_out, node_in, node_out,
                  out,
                  nodes_v, fe_v, fs_v, qe_v, qs_v, ce_v, cs_v, ei_v, eo_v, ni_v, no_v,
                  pools, fh_sent, fh_got, table, news, zs, new_v,
                  sums_v, pair_buf, comb, stage, relay_in, arrive,
                  tab, hsent, qall, oh_q, oh_h, oh_c, oh_p, oh_t, base_v,
                  p16, pair16, comb16, stage16, relay16, arrive16, zt, gpart, gstage, grelay, garrive, ctab,
                  load_sem, edge_sem, fh_s, fh_r, pl_s, pl_r,
                  pair_s, pair_r, rs_s, rs_r, ag_s, ag_r, h_s, h_r,
                  pair16_s, pair16_r, rs16_s, rs16_r, qg_s, qg_r, z_s, z_r, d_s, d_r, g_s, g_r, cg_s, cg_r, store_sem):
    p, me = lax.axis_index("patch"), lax.axis_index("sub")
    core = lax.rem(me, 2)
    x = me // 2
    n_x = n_sub // 2
    partner = {"sub": me + 1 - 2 * core}
    rows = nodes.shape[0]
    degree = f_edges.shape[0]
    tiles = rows // TILE
    q_rows = tab.shape[0] - 2 * W
    share = q_rows // n_sub
    s_rows = p16.shape[0]
    s_share = s_rows // n_sub
    k_q = qs_v.shape[0]
    k_s = cs_v.shape[0]
    send = Sends()

    def column_of(r):
        return lax.rem(x + r, n_x)

    def chip(r):
        return {"sub": 2 * lax.rem(x + r + n_x, n_x) + core}

    def patch(r):
        return {"patch": lax.rem(p + r + n_patch, n_patch)}

    def at(t, size):
        return pl.ds(pl.multiple_of(t * size, size), size)

    def load(src, dst, sem):
        c = pltpu.make_async_copy(src, dst, sem)
        c.start()
        return c

    load_nodes = load(nodes, nodes_v, load_sem.at[0])
    load_ei = load(edge_in, ei_v, load_sem.at[1])
    load_fs = load(f_senders, fs_v, load_sem.at[2])
    for i in range(tiles):
        load(f_edges.at[:, pl.ds(i * TILE, TILE), :], fe_v.at[i], edge_sem.at[i])
    load_rest = [
        load(edge_out, eo_v, load_sem.at[3]),
        load(node_in, ni_v, load_sem.at[4]),
        load(node_out, no_v, load_sem.at[5]),
    ]
    load_later = [
        load(q_edges.at[at(me, share * k_q), :], qe_v, load_sem.at[6]),
        load(q_senders, qs_v, load_sem.at[7]),
        load(c_edges, ce_v, load_sem.at[8]),
        load(c_senders.at[:, at(p, s_rows)], cs_v, load_sem.at[9]),
    ]

    after = {"patch": lax.rem(p + (me + 1) // n_sub, n_patch), "sub": lax.rem(me + 1, n_sub)}
    wrap = (n_sub - me) // n_sub
    before = {"patch": lax.rem(p + n_patch - wrap, n_patch), "sub": lax.rem(me + n_sub - 1, n_sub)}
    peers = [{"sub": lax.rem(me + r, n_sub)} for r in range(1, n_sub)]
    reached = [after, before] + peers + [patch(r) for r in (1, 2, -1, -2)]
    barrier = pltpu.get_barrier_semaphore()
    for to in reached:
        pl.semaphore_signal(barrier, inc=1, device_id=to, device_id_type=MESH)
    pool_rows = pool.shape[0]
    my_pool = pools.at[at(me, pool_rows), :]
    my_pool[...] = pool[...]

    load_nodes.wait()
    raw2 = split2(nodes_v[...])
    for k in range(2):
        fh_sent[k] = halves(dot(one_hot(column(f_halo[k : k + 1, :]), rows), raw2))
    pl.semaphore_wait(barrier, len(reached))
    fine_halo = [
        send(fh_sent.at[k], fh_got.at[k], fh_s.at[k], fh_r.at[k], to) for k, to in ((0, after), (1, before))
    ]
    pool_copies = [send(my_pool, my_pool, pl_s.at[r], pl_r.at[r], to) for r, to in enumerate(peers)]

    load_ei.wait()
    load_fs.wait()
    send_w = packed(ei_v[0, 0:W, :])
    recv_w = packed(ei_v[0, W : 2 * W, :])
    table[0:rows, :] = split2(halves(dot(raw2, send_w)))
    table[rows : rows + 2 * W, :] = packed(ei_v[0, 2 * W : 3 * W, :])

    def sender_columns(i):
        cols = []
        for k in range(degree):
            for j in range(TILE // W):
                cols.append(column(fs_v[k : k + 1, pl.ds(pl.multiple_of(i * TILE + j * W, W), W)]))
        return jnp.concatenate(cols, axis=0)

    def first_pass(i, carry):
        pltpu.make_async_copy(f_edges.at[:, pl.ds(0, TILE), :], fe_v.at[i], edge_sem.at[i]).wait()
        received = mm(nodes_v[at(i, TILE), :], recv_w)
        e2 = jnp.concatenate([split2(fe_v[i, k]) for k in range(degree)], axis=0)
        left = jnp.concatenate([one_hot(sender_columns(i), rows), e2], axis=1)
        zs[i] = halves(dot(left, table[0 : rows + 2 * W, :])) + jnp.concatenate([received] * degree, axis=0)
        return carry

    lax.fori_loop(0, tiles, first_pass, 0)
    for c in load_rest:
        c.wait()

    def level_weights(n):
        node_w = jnp.concatenate([packed(ni_v[n, 0:W, :]), packed(ni_v[n, W : 2 * W, :])], axis=0)
        return packed(centred_columns(eo_v[n])), node_w, packed(centred_columns(no_v[n]))

    out_w, node_w, last_w = level_weights(0)
    for c in fine_halo:
        c.wait_recv()
    halo_table = split2(mm(fh_got[...].reshape(2 * W, W), send_w))

    def second_pass(i, carry):
        hot = one_hot(sender_columns(i) - rows, 2 * W)
        hidden = jnp.maximum(zs[i] + halves(dot(hot, halo_table)), 0.0)
        message = scaled(mm(hidden, out_w))
        summed = fe_v[i, 0] + message[0:TILE]
        for k in range(1, degree):
            summed = summed + (fe_v[i, k] + message[k * TILE : (k + 1) * TILE])
        new = node_update(nodes_v[at(i, TILE), :], summed, node_w, last_w)
        new_v[at(i, TILE), :] = new
        news[at(i, TILE), :] = split2(new)
        return carry

    lax.fori_loop(0, tiles, second_pass, 0)

    class RingSum:
        def __init__(self, part, stage, relay, arrive, ss, rs, half, pieces):
            self.part, self.stage, self.relay, self.arrive = part, stage, relay, arrive
            self.ss, self.rs, self.half, self.pieces = ss, rs, half, pieces
            self.size = half // pieces

        def cut(self, r, h):
            return self.part.at[r, pl.ds(h * self.half, self.half), :]

        def piece(self, i):
            return pl.ds(i * self.size, self.size)

        def part_piece(self, r, h, i):
            return self.part.at[r, pl.ds(h * self.half + i * self.size, self.size), :]

        def far(self):
            self.relayed = {}
            for i in range(self.pieces):
                for h in range(2):
                    k = h * self.pieces + i
                    self.relayed[h, i] = send(self.part_piece(2, h, i), self.relay.at[h, self.piece(i), :],
                                              self.ss.at[k], self.rs.at[k], chip(1 - 2 * h))

        def near(self):
            self.plain = []
            for h in range(2):
                k = 2 * self.pieces + h
                self.plain.append(send(self.cut(1 + 2 * h, 1 - h), self.arrive.at[h, 1 - h], self.ss.at[k],
                                       self.rs.at[k], chip(1 - 2 * h)))

        def pass_on(self):
            self.joint = []
            for i in range(self.pieces):
                for h in range(2):
                    self.relayed[h, i].wait_recv()
                    at_piece = self.piece(i)
                    self.stage[h, at_piece, :] = (
                        self.part_piece(1 + 2 * h, h, i)[...] + self.relay[h, at_piece, :]
                    )
                    k = 2 * self.pieces + 2 + h * self.pieces + i
                    self.joint.append(send(self.stage.at[h, at_piece, :], self.arrive.at[h, h, at_piece, :],
                                           self.ss.at[k], self.rs.at[k], chip(1 - 2 * h)))

        def total(self):
            for c in self.plain + self.joint:
                c.wait_recv()
            return jnp.concatenate(
                [self.cut(0, h)[...] + self.arrive[0, h] + self.arrive[1, h] for h in range(2)], axis=0
            )

    def hot_pool():
        for j in range(rows // W):
            oh_p[j * W : (j + 1) * W, :] = one_hot(column(pool[j : j + 1, :]), q_rows)

    def hot_senders():
        for n, r in enumerate((2, 1, 3, 0)):
            for k in range(k_s):
                g = column(cs_v[k : k + 1, at(column_of(r), W)])
                g = jnp.where(core == 0, g[0:s_share], g[s_share : 2 * s_share])
                g = jnp.where((g // W) % n_x == x, (g // s_rows) * W + g % W, -1)
                first = n * k_s * s_share + k * s_share
                oh_c[first : first + s_share, :] = one_hot(g, n_patch * W)

    def hot_last():
        of_quarter = jnp.concatenate(
            [column(q_pool[j : j + 1, :]).astype(F32) for j in range(q_rows // W)], axis=0
        )
        target = halves(dot(oh_p[...], split2(of_quarter))).astype(jnp.int32)
        oh_t[...] = one_hot(target, s_rows)

    def pair_sum(block, buf, ss, rs, r, size):
        return send(block.at[at(1 - core, size), :], buf.at[r], ss.at[r], rs.at[r], partner)

    pair = {}
    sums = RingSum(comb, stage, relay_in, arrive, rs_s, rs_r, share // 2, 2)
    for r in (2, 1, 3, 0):
        first = pl.multiple_of(column_of(r) * 2 * share, 2 * share)
        sums_v[r] = halves(dot(one_hot_t(pool, first, 2 * share, pool_rows), news[...]))
        pair[r] = pair_sum(sums_v.at[r], pair_buf, pair_s, pair_r, r, share)
        if r == 1:
            pair[2].wait_recv()
            comb[2] = sums_v[2, at(core, share), :] + pair_buf[2]
            sums.far()

    for r in (1, 3):
        pair[r].wait_recv()
        comb[r] = sums_v[r, at(core, share), :] + pair_buf[r]
    sums.near()
    pair[0].wait_recv()
    comb[0] = sums_v[0, at(core, share), :] + pair_buf[0]
    for c in load_later:
        c.wait()
    for k in range(k_q):
        row = qs_v[k : k + 1, at(me, share)]
        col = jnp.concatenate([column(row[:, j * W : (j + 1) * W]) for j in range(share // W)], axis=0)
        oh_q[k * share : (k + 1) * share, :] = one_hot(col, q_rows + 2 * W)
    sums.pass_on()
    for k in range(2):
        oh_h[k * W : (k + 1) * W, :] = one_hot(column(q_halo[k : k + 1, :]), q_rows)
    for c in pool_copies:
        c.wait_recv()
    counts = counts_of(pools, me * share, share, pools.shape[0])
    hot_pool()
    q_send_w = packed(ei_v[1, 0:W, :])
    q = sums.total() / counts
    tab[at(me, share), :] = mm(q, q_send_w)

    class RingGather:
        def __init__(self, buf, ss, rs, size, pieces):
            self.buf, self.ss, self.rs, self.size, self.half = buf, ss, rs, size, size // 2
            self.pieces = pieces
            self.n, self.shared = 0, []
            self.first, self.second = {}, {}
            for i in range(pieces):
                for way in range(2):
                    self.first[way, i] = self.go(0, way, chip(1 - 2 * way), i)
            for way in range(2):
                self.second[way] = self.go(0, 1 - way, chip(1 - 2 * way))
            for h in range(2):
                self.share_half(0, h)

        def go(self, r, h, to, i=None):
            t = 2 * lax.rem(x + r + n_x, n_x) + core
            rows_ = self.half if i is None else self.half // self.pieces
            first = t * self.size + h * self.half + (0 if i is None else i * rows_)
            block = self.buf.at[pl.ds(pl.multiple_of(first, rows_), rows_), :]
            c = send(block, block, self.ss.at[self.n], self.rs.at[self.n], to)
            self.n += 1
            return c

        def share_half(self, r, h, i=None):
            self.shared.append(self.go(r, h, partner, i))

        def pass_on(self):
            self.from_far = {}
            for i in range(self.pieces):
                for way in range(2):
                    self.first[way, i].wait_recv()
                    self.from_far[way, i] = self.go(2 * way - 1, way, chip(1 - 2 * way), i)
            for way in range(2):
                self.share_half(2 * way - 1, way)
            for way in range(2):
                self.second[way].wait_recv()
                self.share_half(2 * way - 1, 1 - way)

        def take_far(self):
            for i in range(self.pieces):
                for way in range(2):
                    self.from_far[way, i].wait_recv()
                    self.share_half(2, way, i)

        def finish(self):
            for c in self.shared:
                c.wait_recv()

    around = RingGather(tab, ag_s, ag_r, share, 2)
    q_recv = mm(q, packed(ei_v[1, W : 2 * W, :]))
    hot_senders()
    around.pass_on()
    edge_w = packed(ei_v[1, 2 * W : 3 * W, :])
    for k in range(k_q):
        base_v[k * share : (k + 1) * share, :] = mm(qe_v[pl.ds(k, share, stride=k_q), :], edge_w) + q_recv
    around.take_far()
    q_out_w, q_node_w, q_last_w = level_weights(1)
    own_pool = q_pool[pl.ds(me * (share // W), share // W), :]
    sub = sublanes(s_rows)
    hot16 = jnp.concatenate(
        [ones_where(jnp.broadcast_to(own_pool[j : j + 1, :], (s_rows, W)) == sub) for j in range(share // W)], axis=1
    )
    around.finish()
    table2 = split2(tab[0:q_rows, :])
    hsent[...] = halves(dot(oh_h[...], table2))
    halo = [
        send(hsent.at[pl.ds(k * W, W), :], tab.at[pl.ds(q_rows + k * W, W), :], h_s.at[k], h_r.at[k], patch(r))
        for k, r in ((0, 1), (1, -1))
    ]
    base = base_v[...] + halves(dot(oh_q[:, 0:q_rows], table2))
    hot_last()
    for c in halo:
        c.wait_recv()
    halo2 = split2(tab[pl.ds(q_rows, 2 * W), :])
    hid = jnp.maximum(base + halves(dot(oh_q[:, q_rows : q_rows + 2 * W], halo2)), 0.0)
    msg = scaled(mm(hid, q_out_w))
    summed = None
    for k in range(k_q):
        term = qe_v[pl.ds(k, share, stride=k_q), :] + msg[k * share : (k + 1) * share]
        summed = term if summed is None else summed + term
    q_new = node_update(q, summed, q_node_w, q_last_w)
    qall[at(me, share), :] = q_new

    p16[...] = halves(dot(hot16, split2(q_new)))
    pair = {}
    for r in (2, 1, 3, 0):
        pair[r] = pair_sum(p16.at[at(column_of(r), 2 * s_share), :], pair16, pair16_s, pair16_r, r, s_share)
    sums = RingSum(comb16, stage16, relay16, arrive16, rs16_s, rs16_r, s_share // 2, 1)
    for r in (2, 1, 3, 0):
        pair[r].wait_recv()
        t = 2 * column_of(r) + core
        comb16[r] = p16[at(t, s_share), :] + pair16[r]
        if r == 2:
            sums.far()
        if r == 3:
            sums.near()
    c_counts = counts_of(q_pool, me * s_share, s_share, q_pool.shape[0])
    c_send_w = packed(ei_v[2, 0:W, :])
    sums.pass_on()
    q_around = RingGather(qall, qg_s, qg_r, share, 1)
    c_recv_w = packed(ei_v[2, W : 2 * W, :])
    c_edge_w = packed(ei_v[2, 2 * W : 3 * W, :])
    c = sums.total() / c_counts
    mine = pl.ds(pl.multiple_of(core * s_share, s_share), s_share)
    zt[p, mine, :] = mm(c, c_send_w)

    arrivals = {}

    def relay(src, sign, dist, last):
        block = zt.at[src, mine, :]
        way = 0 if sign > 0 else 1
        for hop in (2, 1):
            if dist + hop <= last:
                arrivals[sign, dist + hop] = send(
                    block, block, z_s.at[way, dist + hop], z_r.at[way, dist + hop], patch(sign * hop)
                )

    shared = []

    def hand_over(src, slot):
        block = zt.at[src, mine, :]
        shared.append(send(block, block, d_s.at[slot], d_r.at[slot], partner))

    far, near = n_patch // 2, n_patch - n_patch // 2 - 1
    limits = {1: far, -1: near}
    for sign in (1, -1):
        relay(p, sign, 0, limits[sign])
    hand_over(p, 0)

    c_recv = mm(c, c_recv_w)
    c_base = []
    for k in range(k_s):
        c_base.append(mm(ce_v[pl.ds(k, s_share, stride=k_s), :], c_edge_w) + c_recv)

    def add_quarter():
        q_around.finish()
        new_v[...] = new_v[...] + halves(dot(oh_p[...], split2(qall[...])))

    between = {2: q_around.pass_on, 4: q_around.take_far}
    for dist in range(2, far + 2, 2):
        for d in (dist, dist - 1):
            for sign in (1, -1):
                if d <= limits[sign]:
                    arrivals[sign, d].wait_recv()
                    src = lax.rem(p - sign * d + n_patch, n_patch)
                    if d == dist:
                        relay(src, sign, d, limits[sign])
                    hand_over(src, d if sign > 0 else far + d)
        if dist in between:
            between[dist]()
    c_out_w, c_node_w, c_last_w = level_weights(2)
    for s in shared:
        s.wait_recv()
    ztable = split2(zt[...].reshape(n_patch * 2 * s_share, W))
    size = k_s * s_share
    sums = RingSum(gpart, gstage, grelay, garrive, g_s, g_r, size // 2, 2)
    for n, r in enumerate((2, 1, 3, 0)):
        gpart[r] = halves(dot(oh_c[n * size : (n + 1) * size, :], ztable))
        if r == 2:
            sums.far()
        if r == 3:
            sums.near()
    sums.pass_on()
    add_quarter()
    hid = jnp.maximum(jnp.concatenate(c_base, axis=0) + sums.total(), 0.0)
    msg = scaled(mm(hid, c_out_w))
    summed = None
    for k in range(k_s):
        term = ce_v[pl.ds(k, s_share, stride=k_s), :] + msg[k * s_share : (k + 1) * s_share]
        summed = term if summed is None else summed + term
    ctab[at(me, s_share), :] = node_update(c, summed, c_node_w, c_last_w)
    c_around = RingGather(ctab, cg_s, cg_r, s_share, 1)
    c_around.pass_on()
    c_around.take_far()
    c_around.finish()
    ctable = split2(ctab[...])
    stores = []
    for j in range(4):
        block = pl.ds(j * (rows // 4), rows // 4)
        new_v[block, :] = new_v[block, :] + halves(dot(oh_t[block, :], ctable))
        stores.append(load(new_v.at[block, :], out.at[block, :], store_sem.at[j]))
    for c in stores:
        c.wait()
    for s in send.all:
        s.wait_send()


def all_levels(n_patch, n_sub, nodes, f_edges, f_senders, f_halo, pool, q_edges, q_senders, q_halo, q_pool, c_edges,
               c_senders, edge_in, edge_out, node_in, node_out):
    any_ = pl.BlockSpec(memory_space=pl.ANY)
    vm = pl.BlockSpec(memory_space=pltpu.VMEM)
    degree, rows, _ = f_edges.shape
    k_q, q_rows = q_senders.shape
    share = q_rows // n_sub
    k_s = c_senders.shape[0]
    s_rows = c_senders.shape[1] // n_patch
    s_share = s_rows // n_sub
    n_x = n_sub // 2
    dma = pltpu.SemaphoreType.DMA
    v = lambda *shape: pltpu.VMEM(shape, F32)
    b = lambda *shape: pltpu.VMEM(shape, BF)
    i32 = lambda *shape: pltpu.VMEM(shape, jnp.int32)
    gsems = [dma((20,)), dma((20,))]
    return pl.pallas_call(
        functools.partial(levels_kernel, n_patch, n_sub),
        name="all_levels",
        out_shape=jax.ShapeDtypeStruct((rows, W), F32),
        in_specs=[any_, any_, any_, vm, vm, any_, any_, vm, vm, any_, any_, any_, any_, any_, any_],
        out_specs=any_,
        scratch_shapes=[
            v(rows, W), v(rows // TILE, degree, TILE, W), i32(degree, rows),
            v(share * k_q, W), i32(k_q, q_rows), v(s_share * k_s, W), i32(k_s, s_rows),
            v(*edge_in.shape), v(*edge_out.shape), v(*node_in.shape), v(*node_out.shape),
            i32(n_sub * pool.shape[0], W), v(2, W, W), v(2, W, W),
            b(rows + 2 * W, 2 * W), b(rows, 2 * W), v(rows // TILE, degree * TILE, W), v(rows, W),
            v(n_x, 2 * share, W), v(n_x, share, W), v(n_x, share, W),
            v(2, share // 2, W), v(2, share // 2, W), v(2, 2, share // 2, W),
            v(q_rows + 2 * W, W), v(2 * W, W), v(q_rows, W),
            b(k_q * share, q_rows + 2 * W), b(2 * W, q_rows), b(n_x * k_s * s_share, n_patch * W),
            b(rows, q_rows), b(rows, s_rows), v(k_q * share, W),
            v(s_rows, W), v(n_x, s_share, W), v(n_x, s_share, W),
            v(2, s_share // 2, W), v(2, s_share // 2, W), v(2, 2, s_share // 2, W),
            v(n_patch, 2 * s_share, W), v(n_x, k_s * s_share, W),
            v(2, k_s * s_share // 2, W), v(2, k_s * s_share // 2, W), v(2, 2, k_s * s_share // 2, W), v(s_rows, W),
            dma((10,)), dma((rows // TILE,)), dma((2,)), dma((2,)), dma((n_sub - 1,)), dma((n_sub - 1,)),
            dma((n_x,)), dma((n_x,)), dma((10,)), dma((10,)), *gsems, dma((2,)), dma((2,)),
            dma((n_x,)), dma((n_x,)), dma((10,)), dma((10,)), *gsems,
            dma((2, n_patch)), dma((2, n_patch)), dma((n_patch,)), dma((n_patch,)),
            dma((10,)), dma((10,)), *gsems, dma((4,)),
        ],
        compiler_params=pltpu.CompilerParams(collective_id=0, has_side_effects=True, vmem_limit_bytes=VMEM_LIMIT),
    )(nodes, f_edges, f_senders, f_halo, pool, q_edges, q_senders, q_halo, q_pool, c_edges, c_senders, edge_in,
      edge_out, node_in, node_out)


def on_device(n_patch, n_sub, fine_nodes, fine_edges, fine_senders, fine_halo, fine_pool, quarter_edges,
              quarter_senders, quarter_halo, quarter_pool, coarse_edges, coarse_senders, edge_in, edge_out, node_in,
              node_out):
    return all_levels(n_patch, n_sub, fine_nodes, fine_edges.transpose(1, 0, 2), fine_senders.T, fine_halo,
                      fine_pool.reshape(-1, W), quarter_edges.reshape(-1, W), quarter_senders.T, quarter_halo,
                      quarter_pool.reshape(-1, W), coarse_edges.reshape(-1, W), coarse_senders.T, edge_in, edge_out,
                      node_in, node_out)


def solution(mesh):
    both = ("groups", "patch", "sub")
    halfway = ("groups", "patch")
    in_specs = (
        P(both, None),
        P(both, None, None),
        P(both, None),
        P(both, None),
        P(both),
        P(halfway, None, None),
        P(halfway, None),
        P(halfway, None),
        P(halfway),
        P(both, None, None),
        P("groups", None),
        P(),
        P(),
        P(),
        P(),
    )
    return jax.shard_map(
        functools.partial(on_device, mesh.shape["patch"], mesh.shape["sub"]),
        mesh=mesh,
        in_specs=in_specs,
        out_specs=P(both, None),
        check_vma=False,
    )
```

```python
import functools

import jax
import jax.numpy as jnp
from jax import lax
from jax.experimental import pallas as pl
from jax.experimental.pallas import tpu as pltpu
from jax.sharding import PartitionSpec as P

MESH = pl.DeviceIdType.MESH
BF = jnp.bfloat16
F32 = jnp.float32
W = 128
VMEM_LIMIT = 56 * 1024 * 1024


def split2(x):
    hi = x.astype(BF)
    lo = (x - hi.astype(F32)).astype(BF)
    return jnp.concatenate([hi, lo], axis=1)


def packed(w):
    s = split2(w)
    return jnp.concatenate([s, s], axis=0)


def halves(y):
    return y[:, :W] + y[:, W:]


def dot(a, b):
    return jnp.dot(a, b, preferred_element_type=F32)


def mm(x, wp):
    return halves(dot(split2(x), wp))


def centred_columns(w):
    return w - jnp.mean(w, axis=1, keepdims=True)


def scaled(m):
    return m * lax.rsqrt(jnp.mean(m * m, axis=1, keepdims=True) + 1e-05)


def column(row):
    return jnp.broadcast_to(row, (W, W)).T


def lanes(rows):
    return lax.broadcasted_iota(jnp.int32, (rows, W), 1)


def sublanes(rows):
    return lax.broadcasted_iota(jnp.int32, (rows, W), 0)


def ones_where(mask):
    return jnp.where(mask, 1.0, 0.0).astype(BF)


def one_hot(col, width):
    lane = lanes(col.shape[0])
    return jnp.concatenate([ones_where(col == lane + j * W) for j in range(width // W)], axis=1)


def one_hot_t(index_ref, first, rows, blocks):
    sub = sublanes(rows) + first
    return jnp.concatenate(
        [ones_where(jnp.broadcast_to(index_ref[j : j + 1, :], (rows, W)) == sub) for j in range(blocks)],
        axis=1,
    )


def counts_of(index_ref, first, rows, blocks):
    sub = sublanes(rows) + first

    def add(j, acc):
        row = jnp.broadcast_to(index_ref[pl.ds(j, 1), :], (rows, W))
        return acc + jnp.where(row == sub, 1.0, 0.0)

    acc = lax.fori_loop(0, blocks, add, jnp.zeros((rows, W), F32))
    return jnp.sum(acc, axis=1, keepdims=True)


TILE = 512


class Sends:
    def __init__(self):
        self.all = []

    def __call__(self, src, dst, ss, rs, to):
        c = pltpu.make_async_remote_copy(src, dst, ss, rs, device_id=to, device_id_type=MESH)
        c.start()
        self.all.append(c)
        return c


def node_update(h, summed, node_w, last_w):
    both = jnp.concatenate([split2(h), split2(summed)], axis=1)
    a = jnp.maximum(halves(dot(both, node_w)), 0.0)
    return h + scaled(mm(a, last_w))


def levels_kernel(n_patch, n_sub,
                  nodes, f_edges, f_senders, f_halo, pool, q_edges, q_senders, q_halo, q_pool, c_edges, c_senders,
                  edge_in, edge_out, node_in, node_out,
                  out,
                  nodes_v, fe_v, fs_v, qe_v, qs_v, ce_v, cs_v, ei_v, eo_v, ni_v, no_v,
                  pools, fh_sent, fh_got, table, news, zs, new_v,
                  sums_v, pair_buf, comb, stage, relay_in, arrive,
                  tab, hsent, qall, oh_q, oh_h, oh_c, oh_p, oh_t, base_v,
                  p16, pair16, comb16, stage16, relay16, arrive16, zt, gpart, gstage, grelay, garrive, ctab,
                  load_sem, edge_sem, fh_s, fh_r, pl_s, pl_r,
                  pair_s, pair_r, rs_s, rs_r, ag_s, ag_r, h_s, h_r,
                  pair16_s, pair16_r, rs16_s, rs16_r, qg_s, qg_r, z_s, z_r, d_s, d_r, g_s, g_r, cg_s, cg_r, store_sem):
    p, me = lax.axis_index("patch"), lax.axis_index("sub")
    core = lax.rem(me, 2)
    x = me // 2
    n_x = n_sub // 2
    partner = {"sub": me + 1 - 2 * core}
    rows = nodes.shape[0]
    degree = f_edges.shape[0]
    tiles = rows // TILE
    q_rows = tab.shape[0] - 2 * W
    share = q_rows // n_sub
    s_rows = p16.shape[0]
    s_share = s_rows // n_sub
    k_q = qs_v.shape[0]
    k_s = cs_v.shape[0]
    send = Sends()

    def column_of(r):
        return lax.rem(x + r, n_x)

    def chip(r):
        return {"sub": 2 * lax.rem(x + r + n_x, n_x) + core}

    def patch(r):
        return {"patch": lax.rem(p + r + n_patch, n_patch)}

    def at(t, size):
        return pl.ds(pl.multiple_of(t * size, size), size)

    def load(src, dst, sem):
        c = pltpu.make_async_copy(src, dst, sem)
        c.start()
        return c

    load_nodes = load(nodes, nodes_v, load_sem.at[0])
    load_ei = load(edge_in, ei_v, load_sem.at[1])
    load_fs = load(f_senders, fs_v, load_sem.at[2])
    for i in range(tiles):
        load(f_edges.at[:, pl.ds(i * TILE, TILE), :], fe_v.at[i], edge_sem.at[i])
    load_rest = [
        load(edge_out, eo_v, load_sem.at[3]),
        load(node_in, ni_v, load_sem.at[4]),
        load(node_out, no_v, load_sem.at[5]),
    ]
    after = {"patch": lax.rem(p + (me + 1) // n_sub, n_patch), "sub": lax.rem(me + 1, n_sub)}
    wrap = (n_sub - me) // n_sub
    before = {"patch": lax.rem(p + n_patch - wrap, n_patch), "sub": lax.rem(me + n_sub - 1, n_sub)}
    peers = [{"sub": lax.rem(me + r, n_sub)} for r in range(1, n_sub)]
    reached = [after, before] + peers + [patch(r) for r in (1, 2, -1, -2)]
    barrier = pltpu.get_barrier_semaphore()
    for to in reached:
        pl.semaphore_signal(barrier, inc=1, device_id=to, device_id_type=MESH)
    pool_rows = pool.shape[0]
    my_pool = pools.at[at(me, pool_rows), :]
    my_pool[...] = pool[...]

    load_nodes.wait()
    raw2 = split2(nodes_v[...])
    for k in range(2):
        fh_sent[k] = halves(dot(one_hot(column(f_halo[k : k + 1, :]), rows), raw2))
    pl.semaphore_wait(barrier, len(reached))
    fine_halo = [
        send(fh_sent.at[k], fh_got.at[k], fh_s.at[k], fh_r.at[k], to) for k, to in ((0, after), (1, before))
    ]
    pool_copies = [send(my_pool, my_pool, pl_s.at[r], pl_r.at[r], to) for r, to in enumerate(peers)]

    load_later = [
        load(q_edges.at[at(me, share * k_q), :], qe_v, load_sem.at[6]),
        load(q_senders, qs_v, load_sem.at[7]),
        load(c_edges, ce_v, load_sem.at[8]),
        load(c_senders.at[:, at(p, s_rows)], cs_v, load_sem.at[9]),
    ]

    load_ei.wait()
    load_fs.wait()
    send_w = packed(ei_v[0, 0:W, :])
    recv_w = packed(ei_v[0, W : 2 * W, :])
    table[0:rows, :] = split2(halves(dot(raw2, send_w)))
    table[rows : rows + 2 * W, :] = packed(ei_v[0, 2 * W : 3 * W, :])

    def sender_columns(i):
        cols = []
        for k in range(degree):
            for j in range(TILE // W):
                cols.append(column(fs_v[k : k + 1, pl.ds(pl.multiple_of(i * TILE + j * W, W), W)]))
        return jnp.concatenate(cols, axis=0)

    def first_pass(i, carry):
        pltpu.make_async_copy(f_edges.at[:, pl.ds(0, TILE), :], fe_v.at[i], edge_sem.at[i]).wait()
        received = mm(nodes_v[at(i, TILE), :], recv_w)
        e2 = jnp.concatenate([split2(fe_v[i, k]) for k in range(degree)], axis=0)
        left = jnp.concatenate([one_hot(sender_columns(i), rows), e2], axis=1)
        zs[i] = halves(dot(left, table[0 : rows + 2 * W, :])) + jnp.concatenate([received] * degree, axis=0)
        return carry

    lax.fori_loop(0, tiles, first_pass, 0)
    for c in load_rest:
        c.wait()

    def level_weights(n):
        node_w = jnp.concatenate([packed(ni_v[n, 0:W, :]), packed(ni_v[n, W : 2 * W, :])], axis=0)
        return packed(centred_columns(eo_v[n])), node_w, packed(centred_columns(no_v[n]))

    out_w, node_w, last_w = level_weights(0)
    for c in fine_halo:
        c.wait_recv()
    halo_table = split2(mm(fh_got[...].reshape(2 * W, W), send_w))

    def second_pass(i, carry):
        hot = one_hot(sender_columns(i) - rows, 2 * W)
        hidden = jnp.maximum(zs[i] + halves(dot(hot, halo_table)), 0.0)
        message = scaled(mm(hidden, out_w))
        summed = fe_v[i, 0] + message[0:TILE]
        for k in range(1, degree):
            summed = summed + (fe_v[i, k] + message[k * TILE : (k + 1) * TILE])
        new = node_update(nodes_v[at(i, TILE), :], summed, node_w, last_w)
        new_v[at(i, TILE), :] = new
        news[at(i, TILE), :] = split2(new)
        return carry

    lax.fori_loop(0, tiles, second_pass, 0)

    class RingSum:
        def __init__(self, part, stage, relay, arrive, ss, rs, half, pieces):
            self.part, self.stage, self.relay, self.arrive = part, stage, relay, arrive
            self.ss, self.rs, self.half, self.pieces = ss, rs, half, pieces
            self.size = half // pieces

        def cut(self, r, h):
            return self.part.at[r, pl.ds(h * self.half, self.half), :]

        def piece(self, i):
            return pl.ds(i * self.size, self.size)

        def part_piece(self, r, h, i):
            return self.part.at[r, pl.ds(h * self.half + i * self.size, self.size), :]

        def far(self):
            self.relayed = {}
            for i in range(self.pieces):
                for h in range(2):
                    k = h * self.pieces + i
                    self.relayed[h, i] = send(self.part_piece(2, h, i), self.relay.at[h, self.piece(i), :],
                                              self.ss.at[k], self.rs.at[k], chip(1 - 2 * h))

        def near(self):
            self.plain = []
            for h in range(2):
                k = 2 * self.pieces + h
                self.plain.append(send(self.cut(1 + 2 * h, 1 - h), self.arrive.at[h, 1 - h], self.ss.at[k],
                                       self.rs.at[k], chip(1 - 2 * h)))

        def pass_on(self):
            self.joint = []
            for i in range(self.pieces):
                for h in range(2):
                    self.relayed[h, i].wait_recv()
                    at_piece = self.piece(i)
                    self.stage[h, at_piece, :] = (
                        self.part_piece(1 + 2 * h, h, i)[...] + self.relay[h, at_piece, :]
                    )
                    k = 2 * self.pieces + 2 + h * self.pieces + i
                    self.joint.append(send(self.stage.at[h, at_piece, :], self.arrive.at[h, h, at_piece, :],
                                           self.ss.at[k], self.rs.at[k], chip(1 - 2 * h)))

        def total(self):
            for c in self.plain + self.joint:
                c.wait_recv()
            return jnp.concatenate(
                [self.cut(0, h)[...] + self.arrive[0, h] + self.arrive[1, h] for h in range(2)], axis=0
            )

    def hot_pool():
        for j in range(rows // W):
            oh_p[j * W : (j + 1) * W, :] = one_hot(column(pool[j : j + 1, :]), q_rows)

    def hot_senders():
        for n, r in enumerate((2, 1, 3, 0)):
            for k in range(k_s):
                g = column(cs_v[k : k + 1, at(column_of(r), W)])
                g = jnp.where(core == 0, g[0:s_share], g[s_share : 2 * s_share])
                g = jnp.where((g // W) % n_x == x, (g // s_rows) * W + g % W, -1)
                first = n * k_s * s_share + k * s_share
                oh_c[first : first + s_share, :] = one_hot(g, n_patch * W)

    def hot_last():
        of_quarter = jnp.concatenate(
            [column(q_pool[j : j + 1, :]).astype(F32) for j in range(q_rows // W)], axis=0
        )
        target = halves(dot(oh_p[...], split2(of_quarter))).astype(jnp.int32)
        oh_t[...] = one_hot(target, s_rows)

    def pair_sum(block, buf, ss, rs, r, size):
        return send(block.at[at(1 - core, size), :], buf.at[r], ss.at[r], rs.at[r], partner)

    pair = {}
    sums = RingSum(comb, stage, relay_in, arrive, rs_s, rs_r, share // 2, 2)
    for r in (2, 1, 3, 0):
        first = pl.multiple_of(column_of(r) * 2 * share, 2 * share)
        sums_v[r] = halves(dot(one_hot_t(pool, first, 2 * share, pool_rows), news[...]))
        pair[r] = pair_sum(sums_v.at[r], pair_buf, pair_s, pair_r, r, share)
        if r == 1:
            pair[2].wait_recv()
            comb[2] = sums_v[2, at(core, share), :] + pair_buf[2]
            sums.far()

    for r in (1, 3):
        pair[r].wait_recv()
        comb[r] = sums_v[r, at(core, share), :] + pair_buf[r]
    sums.near()
    pair[0].wait_recv()
    comb[0] = sums_v[0, at(core, share), :] + pair_buf[0]
    for c in load_later:
        c.wait()
    for k in range(k_q):
        row = qs_v[k : k + 1, at(me, share)]
        col = jnp.concatenate([column(row[:, j * W : (j + 1) * W]) for j in range(share // W)], axis=0)
        oh_q[k * share : (k + 1) * share, :] = one_hot(col, q_rows + 2 * W)
    sums.pass_on()
    for k in range(2):
        oh_h[k * W : (k + 1) * W, :] = one_hot(column(q_halo[k : k + 1, :]), q_rows)
    for c in pool_copies:
        c.wait_recv()
    counts = counts_of(pools, me * share, share, pools.shape[0])
    hot_pool()
    q_send_w = packed(ei_v[1, 0:W, :])
    q = sums.total() / counts
    tab[at(me, share), :] = mm(q, q_send_w)

    class RingGather:
        def __init__(self, buf, ss, rs, size, pieces):
            self.buf, self.ss, self.rs, self.size, self.half = buf, ss, rs, size, size // 2
            self.pieces = pieces
            self.n, self.shared = 0, []
            self.first, self.second = {}, {}
            for i in range(pieces):
                for way in range(2):
                    self.first[way, i] = self.go(0, way, chip(1 - 2 * way), i)
            for way in range(2):
                self.second[way] = self.go(0, 1 - way, chip(1 - 2 * way))
            for h in range(2):
                self.share_half(0, h)

        def go(self, r, h, to, i=None):
            t = 2 * lax.rem(x + r + n_x, n_x) + core
            rows_ = self.half if i is None else self.half // self.pieces
            first = t * self.size + h * self.half + (0 if i is None else i * rows_)
            block = self.buf.at[pl.ds(pl.multiple_of(first, rows_), rows_), :]
            c = send(block, block, self.ss.at[self.n], self.rs.at[self.n], to)
            self.n += 1
            return c

        def share_half(self, r, h, i=None):
            self.shared.append(self.go(r, h, partner, i))

        def pass_on(self):
            self.from_far = {}
            for i in range(self.pieces):
                for way in range(2):
                    self.first[way, i].wait_recv()
                    self.from_far[way, i] = self.go(2 * way - 1, way, chip(1 - 2 * way), i)
            for way in range(2):
                self.share_half(2 * way - 1, way)
            for way in range(2):
                self.second[way].wait_recv()
                self.share_half(2 * way - 1, 1 - way)

        def take_far(self):
            for i in range(self.pieces):
                for way in range(2):
                    self.from_far[way, i].wait_recv()
                    self.share_half(2, way, i)

        def finish(self):
            for c in self.shared:
                c.wait_recv()

    around = RingGather(tab, ag_s, ag_r, share, 2)
    q_recv = mm(q, packed(ei_v[1, W : 2 * W, :]))
    hot_senders()
    around.pass_on()
    edge_w = packed(ei_v[1, 2 * W : 3 * W, :])
    for k in range(k_q):
        base_v[k * share : (k + 1) * share, :] = mm(qe_v[pl.ds(k, share, stride=k_q), :], edge_w) + q_recv
    around.take_far()
    q_out_w, q_node_w, q_last_w = level_weights(1)
    own_pool = q_pool[pl.ds(me * (share // W), share // W), :]
    sub = sublanes(s_rows)
    hot16 = jnp.concatenate(
        [ones_where(jnp.broadcast_to(own_pool[j : j + 1, :], (s_rows, W)) == sub) for j in range(share // W)], axis=1
    )
    around.finish()
    table2 = split2(tab[0:q_rows, :])
    hsent[...] = halves(dot(oh_h[...], table2))
    halo = [
        send(hsent.at[pl.ds(k * W, W), :], tab.at[pl.ds(q_rows + k * W, W), :], h_s.at[k], h_r.at[k], patch(r))
        for k, r in ((0, 1), (1, -1))
    ]
    base = base_v[...] + halves(dot(oh_q[:, 0:q_rows], table2))
    hot_last()
    for c in halo:
        c.wait_recv()
    halo2 = split2(tab[pl.ds(q_rows, 2 * W), :])
    hid = jnp.maximum(base + halves(dot(oh_q[:, q_rows : q_rows + 2 * W], halo2)), 0.0)
    msg = scaled(mm(hid, q_out_w))
    summed = None
    for k in range(k_q):
        term = qe_v[pl.ds(k, share, stride=k_q), :] + msg[k * share : (k + 1) * share]
        summed = term if summed is None else summed + term
    q_new = node_update(q, summed, q_node_w, q_last_w)
    qall[at(me, share), :] = q_new

    p16[...] = halves(dot(hot16, split2(q_new)))
    pair = {}
    for r in (2, 1, 3, 0):
        pair[r] = pair_sum(p16.at[at(column_of(r), 2 * s_share), :], pair16, pair16_s, pair16_r, r, s_share)
    sums = RingSum(comb16, stage16, relay16, arrive16, rs16_s, rs16_r, s_share // 2, 1)
    for r in (2, 1, 3, 0):
        pair[r].wait_recv()
        t = 2 * column_of(r) + core
        comb16[r] = p16[at(t, s_share), :] + pair16[r]
        if r == 2:
            sums.far()
        if r == 3:
            sums.near()
    c_counts = counts_of(q_pool, me * s_share, s_share, q_pool.shape[0])
    c_send_w = packed(ei_v[2, 0:W, :])
    sums.pass_on()
    q_around = RingGather(qall, qg_s, qg_r, share, 1)
    c_recv_w = packed(ei_v[2, W : 2 * W, :])
    c_edge_w = packed(ei_v[2, 2 * W : 3 * W, :])
    c = sums.total() / c_counts
    mine = pl.ds(pl.multiple_of(core * s_share, s_share), s_share)
    zt[p, mine, :] = mm(c, c_send_w)

    arrivals = {}

    def relay(src, sign, dist, last):
        block = zt.at[src, mine, :]
        way = 0 if sign > 0 else 1
        for hop in (2, 1):
            if dist + hop <= last:
                arrivals[sign, dist + hop] = send(
                    block, block, z_s.at[way, dist + hop], z_r.at[way, dist + hop], patch(sign * hop)
                )

    shared = []

    def hand_over(src, slot):
        block = zt.at[src, mine, :]
        shared.append(send(block, block, d_s.at[slot], d_r.at[slot], partner))

    far, near = n_patch // 2, n_patch - n_patch // 2 - 1
    limits = {1: far, -1: near}
    for sign in (1, -1):
        relay(p, sign, 0, limits[sign])
    hand_over(p, 0)

    c_recv = mm(c, c_recv_w)
    c_base = []
    for k in range(k_s):
        c_base.append(mm(ce_v[pl.ds(k, s_share, stride=k_s), :], c_edge_w) + c_recv)

    def add_quarter():
        q_around.finish()
        new_v[...] = new_v[...] + halves(dot(oh_p[...], split2(qall[...])))

    between = {2: q_around.pass_on, 4: q_around.take_far}
    for dist in range(2, far + 2, 2):
        for d in (dist, dist - 1):
            for sign in (1, -1):
                if d <= limits[sign]:
                    arrivals[sign, d].wait_recv()
                    src = lax.rem(p - sign * d + n_patch, n_patch)
                    if d == dist:
                        relay(src, sign, d, limits[sign])
                    hand_over(src, d if sign > 0 else far + d)
        if dist in between:
            between[dist]()
    c_out_w, c_node_w, c_last_w = level_weights(2)
    for s in shared:
        s.wait_recv()
    ztable = split2(zt[...].reshape(n_patch * 2 * s_share, W))
    size = k_s * s_share
    sums = RingSum(gpart, gstage, grelay, garrive, g_s, g_r, size // 2, 2)
    for n, r in enumerate((2, 1, 3, 0)):
        gpart[r] = halves(dot(oh_c[n * size : (n + 1) * size, :], ztable))
        if r == 2:
            sums.far()
        if r == 3:
            sums.near()
    sums.pass_on()
    add_quarter()
    hid = jnp.maximum(jnp.concatenate(c_base, axis=0) + sums.total(), 0.0)
    msg = scaled(mm(hid, c_out_w))
    summed = None
    for k in range(k_s):
        term = ce_v[pl.ds(k, s_share, stride=k_s), :] + msg[k * s_share : (k + 1) * s_share]
        summed = term if summed is None else summed + term
    ctab[at(me, s_share), :] = node_update(c, summed, c_node_w, c_last_w)
    c_around = RingGather(ctab, cg_s, cg_r, s_share, 1)
    c_around.pass_on()
    c_around.take_far()
    c_around.finish()
    ctable = split2(ctab[...])
    stores = []
    for j in range(4):
        block = pl.ds(j * (rows // 4), rows // 4)
        new_v[block, :] = new_v[block, :] + halves(dot(oh_t[block, :], ctable))
        stores.append(load(new_v.at[block, :], out.at[block, :], store_sem.at[j]))
    for c in stores:
        c.wait()
    for s in send.all:
        s.wait_send()


def all_levels(n_patch, n_sub, nodes, f_edges, f_senders, f_halo, pool, q_edges, q_senders, q_halo, q_pool, c_edges,
               c_senders, edge_in, edge_out, node_in, node_out):
    any_ = pl.BlockSpec(memory_space=pl.ANY)
    vm = pl.BlockSpec(memory_space=pltpu.VMEM)
    degree, rows, _ = f_edges.shape
    k_q, q_rows = q_senders.shape
    share = q_rows // n_sub
    k_s = c_senders.shape[0]
    s_rows = c_senders.shape[1] // n_patch
    s_share = s_rows // n_sub
    n_x = n_sub // 2
    dma = pltpu.SemaphoreType.DMA
    v = lambda *shape: pltpu.VMEM(shape, F32)
    b = lambda *shape: pltpu.VMEM(shape, BF)
    i32 = lambda *shape: pltpu.VMEM(shape, jnp.int32)
    gsems = [dma((20,)), dma((20,))]
    return pl.pallas_call(
        functools.partial(levels_kernel, n_patch, n_sub),
        name="all_levels",
        out_shape=jax.ShapeDtypeStruct((rows, W), F32),
        in_specs=[any_, any_, any_, vm, vm, any_, any_, vm, vm, any_, any_, any_, any_, any_, any_],
        out_specs=any_,
        scratch_shapes=[
            v(rows, W), v(rows // TILE, degree, TILE, W), i32(degree, rows),
            v(share * k_q, W), i32(k_q, q_rows), v(s_share * k_s, W), i32(k_s, s_rows),
            v(*edge_in.shape), v(*edge_out.shape), v(*node_in.shape), v(*node_out.shape),
            i32(n_sub * pool.shape[0], W), v(2, W, W), v(2, W, W),
            b(rows + 2 * W, 2 * W), b(rows, 2 * W), v(rows // TILE, degree * TILE, W), v(rows, W),
            v(n_x, 2 * share, W), v(n_x, share, W), v(n_x, share, W),
            v(2, share // 2, W), v(2, share // 2, W), v(2, 2, share // 2, W),
            v(q_rows + 2 * W, W), v(2 * W, W), v(q_rows, W),
            b(k_q * share, q_rows + 2 * W), b(2 * W, q_rows), b(n_x * k_s * s_share, n_patch * W),
            b(rows, q_rows), b(rows, s_rows), v(k_q * share, W),
            v(s_rows, W), v(n_x, s_share, W), v(n_x, s_share, W),
            v(2, s_share // 2, W), v(2, s_share // 2, W), v(2, 2, s_share // 2, W),
            v(n_patch, 2 * s_share, W), v(n_x, k_s * s_share, W),
            v(2, k_s * s_share // 2, W), v(2, k_s * s_share // 2, W), v(2, 2, k_s * s_share // 2, W), v(s_rows, W),
            dma((10,)), dma((rows // TILE,)), dma((2,)), dma((2,)), dma((n_sub - 1,)), dma((n_sub - 1,)),
            dma((n_x,)), dma((n_x,)), dma((10,)), dma((10,)), *gsems, dma((2,)), dma((2,)),
            dma((n_x,)), dma((n_x,)), dma((10,)), dma((10,)), *gsems,
            dma((2, n_patch)), dma((2, n_patch)), dma((n_patch,)), dma((n_patch,)),
            dma((10,)), dma((10,)), *gsems, dma((4,)),
        ],
        compiler_params=pltpu.CompilerParams(collective_id=0, has_side_effects=True, vmem_limit_bytes=VMEM_LIMIT),
    )(nodes, f_edges, f_senders, f_halo, pool, q_edges, q_senders, q_halo, q_pool, c_edges, c_senders, edge_in,
      edge_out, node_in, node_out)


def on_device(n_patch, n_sub, fine_nodes, fine_edges, fine_senders, fine_halo, fine_pool, quarter_edges,
              quarter_senders, quarter_halo, quarter_pool, coarse_edges, coarse_senders, edge_in, edge_out, node_in,
              node_out):
    return all_levels(n_patch, n_sub, fine_nodes, fine_edges.transpose(1, 0, 2), fine_senders.T, fine_halo,
                      fine_pool.reshape(-1, W), quarter_edges.reshape(-1, W), quarter_senders.T, quarter_halo,
                      quarter_pool.reshape(-1, W), coarse_edges.reshape(-1, W), coarse_senders.T, edge_in, edge_out,
                      node_in, node_out)


def solution(mesh):
    both = ("groups", "patch", "sub")
    halfway = ("groups", "patch")
    in_specs = (
        P(both, None),
        P(both, None, None),
        P(both, None),
        P(both, None),
        P(both),
        P(halfway, None, None),
        P(halfway, None),
        P(halfway, None),
        P(halfway),
        P(both, None, None),
        P("groups", None),
        P(),
        P(),
        P(),
        P(),
    )
    return jax.shard_map(
        functools.partial(on_device, mesh.shape["patch"], mesh.shape["sub"]),
        mesh=mesh,
        in_specs=in_specs,
        out_specs=P(both, None),
        check_vma=False,
    )
```
